32 devices in a mesh: hx: 8 (over z, x), hy: 4 (over y, core).
Axes of the slice: x: 2, y: 2, z: 4, core: 2. Of those that a mesh axis runs over, the one named last changes fastest.
Arguments:
- source: float32 [512, 512], P('hx', 'hy'), may hold values from -27 to 27
- coeffs: float32 [65, 65], replicated, may hold values from -0.13 to 0.13
- row_factor: float32 [512, 512], P('hx'), may hold values from -0.075 to 0.575
- col_factor: float32 [512, 512], P(None, 'hy'), may hold values from -0.075 to 0.575
- tile_mask: int32 [2, 2], replicated, may hold values 0 or 1
Outputs:
- solution: float32 [512, 512], P('hx', 'hy')
- norm_values: float32 [8], replicated
The draws below stay inside these ranges and needn't reach their ends.
Inputs may be any that keep to these rules, and one draw needn't show every extreme that they name: tile_mask[a, b] is 1 where the tile of rows a * 256 onward and columns b * 256 onward carries a block coupling, else 0.
All inputs are finite; a program needn't handle non-finite values.
Results may differ from the reference program's by a relative error of at most 0.0003.
Values sent between devices are 32-bit elements; how exact they have to be, the bound alone decides.
No kernel may reach another device: no remote copies, remote signals or barrier semaphores. Data moves between devices by JAX's collectives and lax.ppermute only.
A program may use at most 64 MiB of HBM per device.

```python
import math
import jax
import jax.numpy as jnp
from jax import lax

TILE = 256
BAND = 32
ITERS = 8
NX = 512
NY = 512


def draw_source(key, part):
    noise_key = jax.random.fold_in(jax.random.fold_in(key, 101), 0)
    col_key = jax.random.fold_in(jax.random.fold_in(key, 101), 2)
    row_place = jnp.arange(NX, dtype=jnp.float32) / NX
    col_level = 10.0 ** jax.random.uniform(col_key, (NY,), jnp.float32)
    noise = jax.random.truncated_normal(noise_key, -4.0, 4.0, (NX, NY), jnp.float32)
    row_level = 10.0 ** row_place
    return noise * row_level[:, None] * col_level[None, :] / 15.0


def draw_coeffs(key, part):
    tap_count = 2 * BAND + 1
    noise_key = jax.random.fold_in(key, 202)
    offsets = jnp.abs(jnp.arange(tap_count, dtype=jnp.float32) - BAND)
    decay = 0.03 / jnp.sqrt((1.0 + offsets)[:, None] * (1.0 + offsets)[None, :])
    noise = jax.random.truncated_normal(noise_key, -4.0, 4.0, (tap_count, tap_count), jnp.float32)
    return noise * decay


def diagonal_part():
    same_place = jnp.arange(NX)[:, None] % TILE == jnp.arange(NY)[None, :] % TILE
    return 0.5 * same_place.astype(jnp.float32)


def draw_row_factor(key, part):
    noise_key = jax.random.fold_in(key, 303)
    noise = jax.random.truncated_normal(noise_key, -4.0, 4.0, (NX, NY), jnp.float32)
    return diagonal_part() + 0.3 * noise / math.sqrt(TILE)


def draw_col_factor(key, part):
    noise_key = jax.random.fold_in(key, 404)
    noise = jax.random.truncated_normal(noise_key, -4.0, 4.0, (NX, NY), jnp.float32)
    return diagonal_part() + 0.3 * noise / math.sqrt(TILE)


def plant(values, key, least, largest):
    dims = values.shape
    index_at = [jax.random.randint(jax.random.fold_in(key, axis), (), 0, dims[axis]) for axis in range(len(dims))]
    values = values.at[tuple(index_at)].set(least)
    longest = dims.index(max(dims))
    index_at[longest] = (index_at[longest] + 1) % dims[longest]
    return values.at[tuple(index_at)].set(largest)


def setup_inputs(seed: int = 0) -> dict:
    key_of = jax.random.split(jax.random.key(seed), 6)
    return {
        "source": draw_source(jax.random.fold_in(key_of[5], 71), 0),
        "coeffs": draw_coeffs(jax.random.fold_in(key_of[5], 71), 0),
        "row_factor": draw_row_factor(jax.random.fold_in(key_of[5], 71), 0),
        "col_factor": draw_col_factor(jax.random.fold_in(key_of[5], 71), 0),
        "tile_mask": plant((jax.random.randint(key_of[4], (NX // TILE, NY // TILE), 0, 2) < 1).astype(jnp.int32), jax.random.fold_in(key_of[4], 1), 0, 1),
    }


relax_step = 0.25
highest = lax.Precision.HIGHEST
tiny_square = 1e-06

def banded_product(field_now, coeffs):
    band_width = (coeffs.shape[0] - 1) // 2
    row_count, col_count = field_now.shape
    full_shape = (row_count + 2 * band_width, col_count + 2 * band_width)
    spectrum = jnp.fft.rfft2(field_now, s=full_shape) * jnp.fft.rfft2(coeffs, s=full_shape)
    full_conv = jnp.fft.irfft2(spectrum, s=full_shape)
    return full_conv[band_width:band_width + row_count, band_width:band_width + col_count]

def tile_term(field_now, row_factor, col_factor, tile_mask):
    tiles_down, tiles_across = tile_mask.shape
    shape_four = (tiles_down, TILE, tiles_across, TILE)
    mixed = jnp.einsum('aibj,ajbl->aibl', row_factor.reshape(shape_four), field_now.reshape(shape_four), precision=highest)
    result = jnp.einsum('aibk,akbl->aibl', mixed, col_factor.reshape(shape_four), precision=highest)
    weights = tile_mask.astype(jnp.float32)[:, None, :, None]
    return (result * weights).reshape(field_now.shape)

def reference(source, coeffs, row_factor, col_factor, tile_mask):
    solution = source
    squares = []
    for step_index in range(ITERS):
        applied = solution + banded_product(solution, coeffs) + tile_term(solution, row_factor, col_factor, tile_mask)
        residual = source - applied
        squares.append(jnp.sum(residual * residual))
        solution = solution + relax_step * residual
    norm_values = jnp.sqrt(jnp.stack(squares) / (NX * NY) + tiny_square)
    return (solution, norm_values)
```

```python
import functools
import jax
import jax.numpy as jnp
import numpy as np
from jax import lax
from jax.experimental import pallas as pl
from jax.experimental.pallas import tpu as pltpu
from jax.sharding import PartitionSpec as P

TILE = 256
ITERS = 8
HALF = TILE // 2
LANES = 128
GRID_BYTES = 2 * 1024 * 1024


relax_step = 0.25
highest = lax.Precision.HIGHEST
tiny_square = 1e-06


def with_halo(value, sides, width):
    for axis, dim in sides:
        count, length = (lax.axis_size(axis), value.shape[dim])
        up = [(i, (i + 1) % count) for i in range(count - 1)]
        down = [(j, i) for i, j in up]
        last = lax.slice_in_dim(value, length - width, length, axis=dim)
        initial = lax.slice_in_dim(value, 0, width, axis=dim)
        before = lax.ppermute(last, axis, up)
        after = lax.ppermute(initial, axis, down)
        value = jnp.concatenate([before, value, after], axis=dim)
    return value


def swapped(value, axis, apart):
    return lax.ppermute(value, axis, [(i, i ^ 1 << apart) for i in range(lax.axis_size(axis))])


def row_panels(coeffs, row_count, band_width):
    tap_count = 2 * band_width + 1
    padded_rows = row_count + 2 * band_width
    shape_three = (tap_count, row_count, padded_rows)
    tap_index = lax.broadcasted_iota(jnp.int32, shape_three, 0)
    target = lax.broadcasted_iota(jnp.int32, shape_three, 1)
    source_row = lax.broadcasted_iota(jnp.int32, shape_three, 2)
    picker = (source_row == target + 2 * band_width - tap_index).astype(jnp.float32)
    panels = jnp.einsum("pq,pmi->mqi", coeffs, picker, precision=highest)
    return panels.reshape(row_count, tap_count * padded_rows)


def banded_product(field_now, panels, band_width):
    col_count = field_now.shape[1]
    padded = with_halo(field_now, (("hx", 0), ("hy", 1)), band_width)
    pieces = [
        padded[:, 2 * band_width - offset : 2 * band_width - offset + col_count]
        for offset in range(2 * band_width + 1)
    ]
    stacked = jnp.concatenate(pieces, axis=0)
    return jnp.dot(panels, stacked, precision=highest, preferred_element_type=jnp.float32)


def joined(block, partner, upper_half, axis_dim):
    return jnp.where(
        upper_half,
        jnp.concatenate([partner, block], axis_dim),
        jnp.concatenate([block, partner], axis_dim),
    )


def distributed(source, coeffs, row_factor, col_factor, tile_mask):
    row_count, col_count = source.shape
    band_width = (coeffs.shape[0] - 1) // 2
    row_group = TILE // row_count
    col_group = TILE // col_count
    row_index = lax.axis_index("hx")
    col_index = lax.axis_index("hy")
    tile_row = row_index // row_group
    tile_col = col_index // col_group
    panels = row_panels(coeffs, row_count, band_width)
    row_factor_tile = lax.dynamic_slice_in_dim(row_factor, tile_col * TILE, TILE, 1)
    col_factor_tile = lax.dynamic_slice_in_dim(col_factor, tile_row * TILE, TILE, 0)
    mask_rows = lax.broadcasted_iota(jnp.int32, tile_mask.shape, 0)
    mask_cols = lax.broadcasted_iota(jnp.int32, tile_mask.shape, 1)
    chosen = (mask_rows == tile_row) & (mask_cols == tile_col)
    active = jnp.sum(jnp.where(chosen, tile_mask, 0)).astype(jnp.float32)
    solution = source
    squares = []
    for step_index in range(ITERS):
        wide_block = solution
        bit_level = 0
        partner = swapped(wide_block, "hy", bit_level)
        upper_half = col_index // (1 << bit_level) % 2 == 1
        wide_block = joined(wide_block, partner, upper_half, 1)
        mixed_cols = jnp.dot(
            wide_block, col_factor_tile, precision=highest, preferred_element_type=jnp.float32
        )
        tall_block = mixed_cols
        for bit_level in range(row_group.bit_length() - 1):
            partner = swapped(tall_block, "hx", bit_level)
            upper_half = row_index // (1 << bit_level) % 2 == 1
            tall_block = joined(tall_block, partner, upper_half, 0)
        result = jnp.dot(
            row_factor_tile, tall_block, precision=highest, preferred_element_type=jnp.float32
        )
        applied = solution + banded_product(solution, panels, band_width) + active * result
        residual = source - applied
        local_square = jnp.sum(residual * residual)
        squares.append(lax.psum(local_square, ("hx", "hy")))
        solution = solution + relax_step * residual
    summed = jnp.stack(squares)
    cell_count = row_count * col_count * lax.axis_size("hx") * lax.axis_size("hy")
    norm_values = jnp.sqrt(summed / cell_count + tiny_square)
    return (solution, norm_values)


def packed_dft():
    place = np.arange(TILE)
    freq = np.arange(HALF)
    phase = 2 * np.pi * ((freq[:, None] * place[None, :]) % TILE) / TILE
    forward = np.concatenate([np.cos(phase), np.sin(phase)], 0)
    forward[HALF] = np.cos(np.pi * place)
    weight = np.full((TILE, 1), 2.0 / TILE)
    weight[0] = weight[HALF] = 1.0 / TILE
    return forward, (forward * weight).T


def tap_waves(band_width):
    offset = np.arange(-band_width, band_width + 1)
    freq = np.concatenate([np.arange(HALF), np.arange(HALF)])
    freq[HALF] = HALF
    phase = 2 * np.pi * ((freq[:, None] * offset[None, :]) % TILE) / TILE
    return np.concatenate([np.cos(phase), np.sin(phase)], 0).astype(np.float32)


def split_np(value):
    high = value.astype(jnp.bfloat16)
    return high, (value - high.astype(np.float64)).astype(jnp.bfloat16)


def window_mats(length, band_width):
    forward, inverse = packed_dft()
    count = length // HALF - 1
    mats = [[], [], [], []]
    spans = []
    for w in range(count):
        first, last = w == 0, w == count - 1
        taken = np.ones(TILE)
        if first:
            taken[TILE - band_width :] = 0
        if last:
            taken[:band_width] = 0
        low = 0 if first else HALF // 2
        high = TILE if last else TILE - HALF // 2
        spans.append((low, high))
        kept = np.zeros(TILE)
        kept[low:high] = 1
        fh, fl = split_np(forward * taken[None, :])
        gh, gl = split_np(inverse * kept[:, None])
        mats[0].append(np.concatenate([fh, fh, fl], 1))
        mats[1].append(np.concatenate([fh.T, fh.T, fl.T], 0))
        mats[2].append(np.concatenate([gh, gh, gl], 1))
        mats[3].append(np.concatenate([gh.T, gh.T, gl.T], 0))
    return [np.stack(m) for m in mats], spans


def tap_spectrum(coeffs):
    waves = jnp.asarray(tap_waves((coeffs.shape[0] - 1) // 2))
    mixed = jnp.dot(jnp.dot(waves, coeffs, precision=highest), waves.T, precision=highest)
    sign = np.where(np.arange(TILE) < HALF, -1.0, 1.0).astype(np.float32)
    quarter = [[mixed[i * TILE : (i + 1) * TILE, j * TILE : (j + 1) * TILE] for j in (0, 1)] for i in (0, 1)]
    return jnp.stack(
        [
            quarter[0][0],
            quarter[1][0] * sign[:, None],
            quarter[0][1] * sign[None, :],
            quarter[1][1] * (sign[:, None] * sign[None, :]),
        ]
    )


def split(value):
    high = value.astype(jnp.bfloat16)
    return high, (value - high.astype(jnp.float32)).astype(jnp.bfloat16)


def dot32(left, right):
    return jnp.dot(left, right, preferred_element_type=jnp.float32)


def replicated_kernel(
    row_spans, hx_bits, col_places, place, mask, s_own, s_far, r_own, r_far, c_own, c_far, spectrum,
    row_fwd, col_fwd, row_inv, col_inv, out, squares,
    state, total, w_hi, w_lo, z_hi, z_lo, y_hi, y_lo, u_hi, u_lo, t_hi, t_lo, wave, left, right,
):
    rows, cols = state.shape
    row_windows, col_windows = row_fwd.shape[0], col_fwd.shape[0]
    tile_rows, tile_cols = rows // TILE, cols // TILE
    block_rows, block_cols = s_own.shape[-2:]
    here_x, here_y, here_c = place[0], place[1], place[2]
    for pos in range(s_own.shape[0]):
        s_row = (here_x ^ hx_bits[0][pos]) * block_rows
        s_row = pl.multiple_of(s_row, block_rows)
        for far, ref in ((0, s_own), (1, s_far)):
            for k in range(s_own.shape[1]):
                s_col = ((here_y ^ k) * 2 + (here_c ^ far)) * block_cols
                s_col = pl.multiple_of(s_col, block_cols)
                value = ref[pos, k]
                state[pl.ds(s_row, block_rows), pl.ds(s_col, block_cols)] = value
                total[pl.ds(s_row, block_rows), pl.ds(s_col, block_cols)] = value
                high, low = split(value)
                w_hi[pl.ds(s_row, block_rows), pl.ds(s_col, block_cols)] = high
                w_lo[pl.ds(s_row, block_rows), pl.ds(s_col, block_cols)] = low
    share = TILE // block_rows
    for pos in range(r_own.shape[0]):
        index = here_x ^ hx_bits[1][pos]
        a = index // share
        sub = pl.multiple_of((index % share) * block_rows, block_rows)
        for far, ref in ((0, r_own), (1, r_far)):
            side = here_c ^ far
            for k in range(r_own.shape[1]):
                lane = side * (cols // 2) + k * LANES
                b = lane // TILE
                at = pl.multiple_of(lane % TILE, LANES)
                high, low = split(ref[pos, k] * mask[a, b].astype(jnp.float32))
                for third, part in enumerate((high, high, low)):
                    left[a, b, pl.ds(sub, block_rows), pl.ds(pl.multiple_of(at + third * TILE, LANES), LANES)] = part
    for k in range(c_own.shape[0]):
        for far, ref in ((0, c_own), (1, c_far)):
            lane = ((here_y ^ k) * 2 + (here_c ^ far)) * block_cols
            b = lane // TILE
            at = pl.multiple_of(lane % TILE, block_cols)
            for a in range(tile_rows):
                high, low = split(ref[k, pl.ds(a * TILE, TILE), :])
                for third, part in enumerate((high, high, low)):
                    right[a, b, pl.ds(third * TILE, TILE), pl.ds(at, block_cols)] = part

    def triple(hi_ref, lo_ref, row_at, col_at, axis):
        high = hi_ref[row_at, col_at]
        return jnp.concatenate([high, lo_ref[row_at, col_at], high], axis)

    def step(k, carry):
        keep = jnp.where(k == 0, 0.0, 1.0 - relax_step)
        take = jnp.where(k == 0, 1.0, relax_step)
        every = pl.ds(0, rows)
        for b in range(col_windows):
            z = dot32(triple(w_hi, w_lo, every, pl.ds(b * HALF, TILE), 1), col_fwd[b])
            z_hi[:, pl.ds(b * TILE, TILE)], z_lo[:, pl.ds(b * TILE, TILE)] = split(z)
        for a in range(row_windows):
            for b in range(col_windows):
                cells = triple(z_hi, z_lo, pl.ds(a * HALF, TILE), pl.ds(b * TILE, TILE), 0)
                wave[...] = dot32(row_fwd[a], cells)
                for i in (0, 1):
                    for j in (0, 1):
                        ri, rj = pl.ds(i * HALF, HALF), pl.ds((1 - i) * HALF, HALF)
                        ci, cj = pl.ds(j * HALF, HALF), pl.ds((1 - j) * HALF, HALF)
                        y = (
                            spectrum[0, ri, ci] * wave[ri, ci]
                            + spectrum[1, ri, ci] * wave[rj, ci]
                            + spectrum[2, ri, ci] * wave[ri, cj]
                            + spectrum[3, ri, ci] * wave[rj, cj]
                        )
                        to = pl.ds(a * TILE + i * HALF, HALF), pl.ds(b * TILE + j * HALF, HALF)
                        y_hi[to], y_lo[to] = split(y)
        for a in range(row_windows):
            low, high = row_spans[a]
            for b in range(col_windows):
                cells = triple(y_hi, y_lo, pl.ds(a * TILE, TILE), pl.ds(b * TILE, TILE), 0)
                u = dot32(row_inv[a, low:high, :], cells)
                to = pl.ds(a * HALF + low, high - low), pl.ds(b * TILE, TILE)
                u_hi[to], u_lo[to] = split(u)
        for a in range(tile_rows):
            for b in range(tile_cols):
                at = pl.ds(a * TILE, TILE), pl.ds(b * TILE, TILE)
                t_hi[at], t_lo[at] = split(dot32(left[a, b], triple(w_hi, w_lo, *at, 0)))
        square = jnp.zeros((8, LANES), jnp.float32)
        for a in range(tile_rows):
            ra = pl.ds(a * TILE, TILE)
            parts = []
            for b in range(col_windows):
                lhs = triple(u_hi, u_lo, ra, pl.ds(b * TILE, TILE), 1)
                rhs = col_inv[b]
                if b % 2 == 0:
                    lhs = jnp.concatenate([lhs, triple(t_hi, t_lo, ra, pl.ds(b // 2 * TILE, TILE), 1)], 1)
                    rhs = jnp.concatenate([rhs, right[a, b // 2]], 0)
                parts.append(dot32(lhs, rhs))
            for j in range(cols // HALF):
                pieces = [parts[b][:, (j - b) * HALF : (j - b + 1) * HALF] for b in range(col_windows) if b <= j <= b + 1]
                cj = pl.ds(j * HALF, HALF)
                residual = keep * state[ra, cj] - take * functools.reduce(jnp.add, pieces)
                state[ra, cj] = residual
                total[ra, cj] = total[ra, cj] + relax_step * residual
                w_hi[ra, cj], w_lo[ra, cj] = split(residual)
                square = square + jnp.sum((residual * residual).reshape(TILE // 8, 8, LANES), 0)
        squares[k] = square
        return carry

    lax.fori_loop(0, ITERS, step, 0)
    own_row = pl.multiple_of(here_x * block_rows, block_rows)
    own_col = pl.multiple_of((here_y * 2 + here_c) * block_cols, block_cols)
    out[...] = total[pl.ds(own_row, block_rows), pl.ds(own_col, block_cols)]


def swap(value, axis, bit):
    return lax.ppermute(value, axis, [(i, i ^ bit) for i in range(lax.axis_size(axis))])


def doubled(value, axis, bits):
    for bit in bits:
        value = jnp.concatenate([value, swap(value, axis, bit)], 0)
    return value


def bit_places(bits):
    places = [0]
    for bit in bits:
        places = places + [p | bit for p in places]
    return places


def replicated(source, coeffs, row_factor, col_factor, tile_mask):
    block_rows, block_cols = source.shape
    rows, cols = col_factor.shape[0], row_factor.shape[1]
    band_width = (coeffs.shape[0] - 1) // 2
    hx_size, hy_size = lax.axis_size("hx"), lax.axis_size("hy")
    index_x, index_y = lax.axis_index("hx"), lax.axis_index("hy")
    down = [1 << i for i in reversed(range(hx_size.bit_length() - 1))]
    turned = down[:-2] + down[-2:][::-1]
    y_bits = [1 << i for i in range(1, hy_size.bit_length() - 1)]
    s_part = doubled(source[None], "hy", y_bits)
    c_part = doubled(col_factor[None], "hy", y_bits)
    r_half = lax.dynamic_slice_in_dim(row_factor, (index_y % 2) * (cols // 2), cols // 2, 1)
    r_part = r_half.reshape(block_rows, -1, LANES).swapaxes(0, 1)
    s_count = s_part.shape[0]
    both = jnp.concatenate([s_part, r_part], 0)[None]
    both = doubled(both, "hx", down[:-2])
    s_all = doubled(both[:, :s_count], "hx", down[-2:])
    r_all = doubled(both[:, s_count:], "hx", turned[-2:])
    far = [swap(v, "hy", 1) for v in (s_all, r_all, c_part)]
    spectrum = tap_spectrum(coeffs)
    mats, row_spans = window_mats(rows, band_width)
    col_mats, _ = window_mats(cols, band_width)
    weights = [jnp.asarray(m) for m in (mats[0], col_mats[1], mats[2], col_mats[3])]
    place = jnp.stack([index_x, index_y // 2, index_y % 2])
    row_windows, col_windows = rows // HALF - 1, cols // HALF - 1
    vmem = pl.BlockSpec(memory_space=pltpu.VMEM)
    smem = pl.BlockSpec(memory_space=pltpu.SMEM)
    f32, bf16 = jnp.float32, jnp.bfloat16
    shapes = [((rows, cols), f32)] * 2 + [((rows, cols), bf16)] * 2 + [((rows, col_windows * TILE), bf16)] * 2
    shapes += [((row_windows * TILE, col_windows * TILE), bf16)] * 2 + [((rows, col_windows * TILE), bf16)] * 2
    shapes += [((rows, cols), bf16)] * 2 + [((TILE, TILE), f32)]
    tiles = (rows // TILE, cols // TILE)
    shapes += [(tiles + (TILE, 3 * TILE), bf16), (tiles + (3 * TILE, TILE), bf16)]
    result, squares = pl.pallas_call(
        functools.partial(replicated_kernel, row_spans, (bit_places(down), bit_places(turned)), None),
        out_shape=(
            jax.ShapeDtypeStruct((block_rows, block_cols), f32),
            jax.ShapeDtypeStruct((ITERS, 8, LANES), f32),
        ),
        in_specs=[smem, smem] + [vmem] * 11,
        out_specs=(vmem, vmem),
        scratch_shapes=[pltpu.VMEM(*s) for s in shapes],
        compiler_params=pltpu.CompilerParams(vmem_limit_bytes=40 * 1024 * 1024),
        name="replicated_steps",
    )(place, tile_mask, s_all, far[0], r_all, far[1], c_part, far[2], spectrum, *weights)
    norm_values = jnp.sqrt(jnp.sum(squares, (1, 2)) / (rows * cols) + tiny_square)
    return result, norm_values


def fits(rows, cols, block_rows, block_cols, band_width, hx_size, hy_size):
    powers = all(n & (n - 1) == 0 for n in (hx_size, hy_size))
    whole = rows % TILE == 0 and cols % TILE == 0 and rows > TILE and cols > TILE
    aligned = TILE % block_rows == 0 and block_rows % 16 == 0 and block_cols == LANES and cols % (2 * LANES) == 0
    small = rows * cols * 4 <= GRID_BYTES and 4 * band_width <= TILE
    return powers and whole and aligned and small and hx_size >= 4 and hy_size >= 2


def local(source, coeffs, row_factor, col_factor, tile_mask):
    rows, cols = col_factor.shape[0], row_factor.shape[1]
    band_width = (coeffs.shape[0] - 1) // 2
    sizes = lax.axis_size("hx"), lax.axis_size("hy")
    if fits(rows, cols, *source.shape, band_width, *sizes):
        return replicated(source, coeffs, row_factor, col_factor, tile_mask)
    return distributed(source, coeffs, row_factor, col_factor, tile_mask)


def solution(mesh):
    in_specs = (P("hx", "hy"), P(), P("hx", None), P(None, "hy"), P())
    out_specs = (P("hx", "hy"), P())
    return jax.shard_map(local, mesh=mesh, in_specs=in_specs, out_specs=out_specs, check_vma=False)
```

```python
import functools
import jax
import jax.numpy as jnp
import numpy as np
from jax import lax
from jax.experimental import pallas as pl
from jax.experimental.pallas import tpu as pltpu
from jax.sharding import PartitionSpec as P

TILE = 256
ITERS = 8
HALF = TILE // 2
LANES = 128
GRID_BYTES = 2 * 1024 * 1024


relax_step = 0.25
highest = lax.Precision.HIGHEST
tiny_square = 1e-06


def with_halo(value, sides, width):
    for axis, dim in sides:
        count, length = (lax.axis_size(axis), value.shape[dim])
        up = [(i, (i + 1) % count) for i in range(count - 1)]
        down = [(j, i) for i, j in up]
        last = lax.slice_in_dim(value, length - width, length, axis=dim)
        initial = lax.slice_in_dim(value, 0, width, axis=dim)
        before = lax.ppermute(last, axis, up)
        after = lax.ppermute(initial, axis, down)
        value = jnp.concatenate([before, value, after], axis=dim)
    return value


def swapped(value, axis, apart):
    return lax.ppermute(value, axis, [(i, i ^ 1 << apart) for i in range(lax.axis_size(axis))])


def row_panels(coeffs, row_count, band_width):
    tap_count = 2 * band_width + 1
    padded_rows = row_count + 2 * band_width
    shape_three = (tap_count, row_count, padded_rows)
    tap_index = lax.broadcasted_iota(jnp.int32, shape_three, 0)
    target = lax.broadcasted_iota(jnp.int32, shape_three, 1)
    source_row = lax.broadcasted_iota(jnp.int32, shape_three, 2)
    picker = (source_row == target + 2 * band_width - tap_index).astype(jnp.float32)
    panels = jnp.einsum("pq,pmi->mqi", coeffs, picker, precision=highest)
    return panels.reshape(row_count, tap_count * padded_rows)


def banded_product(field_now, panels, band_width):
    col_count = field_now.shape[1]
    padded = with_halo(field_now, (("hx", 0), ("hy", 1)), band_width)
    pieces = [
        padded[:, 2 * band_width - offset : 2 * band_width - offset + col_count]
        for offset in range(2 * band_width + 1)
    ]
    stacked = jnp.concatenate(pieces, axis=0)
    return jnp.dot(panels, stacked, precision=highest, preferred_element_type=jnp.float32)


def joined(block, partner, upper_half, axis_dim):
    return jnp.where(
        upper_half,
        jnp.concatenate([partner, block], axis_dim),
        jnp.concatenate([block, partner], axis_dim),
    )


def distributed(source, coeffs, row_factor, col_factor, tile_mask):
    row_count, col_count = source.shape
    band_width = (coeffs.shape[0] - 1) // 2
    row_group = TILE // row_count
    col_group = TILE // col_count
    row_index = lax.axis_index("hx")
    col_index = lax.axis_index("hy")
    tile_row = row_index // row_group
    tile_col = col_index // col_group
    panels = row_panels(coeffs, row_count, band_width)
    row_factor_tile = lax.dynamic_slice_in_dim(row_factor, tile_col * TILE, TILE, 1)
    col_factor_tile = lax.dynamic_slice_in_dim(col_factor, tile_row * TILE, TILE, 0)
    mask_rows = lax.broadcasted_iota(jnp.int32, tile_mask.shape, 0)
    mask_cols = lax.broadcasted_iota(jnp.int32, tile_mask.shape, 1)
    chosen = (mask_rows == tile_row) & (mask_cols == tile_col)
    active = jnp.sum(jnp.where(chosen, tile_mask, 0)).astype(jnp.float32)
    solution = source
    squares = []
    for step_index in range(ITERS):
        wide_block = solution
        bit_level = 0
        partner = swapped(wide_block, "hy", bit_level)
        upper_half = col_index // (1 << bit_level) % 2 == 1
        wide_block = joined(wide_block, partner, upper_half, 1)
        mixed_cols = jnp.dot(
            wide_block, col_factor_tile, precision=highest, preferred_element_type=jnp.float32
        )
        tall_block = mixed_cols
        for bit_level in range(row_group.bit_length() - 1):
            partner = swapped(tall_block, "hx", bit_level)
            upper_half = row_index // (1 << bit_level) % 2 == 1
            tall_block = joined(tall_block, partner, upper_half, 0)
        result = jnp.dot(
            row_factor_tile, tall_block, precision=highest, preferred_element_type=jnp.float32
        )
        applied = solution + banded_product(solution, panels, band_width) + active * result
        residual = source - applied
        local_square = jnp.sum(residual * residual)
        squares.append(lax.psum(local_square, ("hx", "hy")))
        solution = solution + relax_step * residual
    summed = jnp.stack(squares)
    cell_count = row_count * col_count * lax.axis_size("hx") * lax.axis_size("hy")
    norm_values = jnp.sqrt(summed / cell_count + tiny_square)
    return (solution, norm_values)


def split_np(value):
    high = value.astype(jnp.bfloat16)
    return high, (value - high.astype(np.float64)).astype(jnp.bfloat16)


def packed_freqs(length):
    half = length // 2
    freq = np.concatenate([np.arange(half), np.arange(half)])
    freq[half] = half
    return freq


def cyclic_mats(length):
    half = length // 2
    phase = 2 * np.pi * ((packed_freqs(length)[:, None] * np.arange(length)[None, :]) % length) / length
    forward = np.concatenate([np.cos(phase[: half + 1]), np.sin(phase[half + 1 :])], 0)
    weight = np.full((length, 1), 2.0 / length)
    weight[0] = weight[half] = 1.0 / length
    return forward, (forward * weight).T


def negacyclic_mats(length):
    half = length // 2
    odd = 2 * np.arange(half) + 1
    phase = 2 * np.pi * ((odd[:, None] * np.arange(length)[None, :]) % (2 * length)) / (2 * length)
    forward = np.concatenate([np.cos(phase), np.sin(phase)], 0)
    return forward, (forward * (2.0 / length)).T


def row_mats(band_width):
    half = (TILE + 2 * band_width) // 2
    fwd, inv = [], []
    for forward, inverse in (cyclic_mats(half), negacyclic_mats(half)):
        fh, fl = split_np(forward)
        gh, gl = split_np(inverse * 0.5)
        fwd.append(np.concatenate([fh, fh, fl], 1))
        inv.append(np.concatenate([gh, gh, gl], 1))
    return np.stack(fwd), np.stack(inv)


def col_mats():
    forward, inverse = cyclic_mats(TILE)
    return np.stack(split_np(forward.T) + split_np(inverse.T))


def tap_waves(band_width):
    offset = np.arange(-band_width, band_width + 1)
    half = (TILE + 2 * band_width) // 2
    odd = 2 * np.arange(half // 2) + 1
    row_freq = np.concatenate([2 * packed_freqs(half), odd, odd])
    row_phase = 2 * np.pi * ((row_freq[:, None] * offset[None, :]) % (2 * half)) / (2 * half)
    col_phase = 2 * np.pi * ((packed_freqs(TILE)[:, None] * offset[None, :]) % TILE) / TILE
    rows = np.stack([np.cos(row_phase), np.sin(row_phase)]).astype(np.float32)
    cols = np.stack([np.cos(col_phase).T, np.sin(col_phase).T]).astype(np.float32)
    return rows, cols


def setup_kernel(coeffs, row_waves, col_waves, col_base, spectrum, col_fwd, col_inv):
    half = spectrum.shape[2]
    band_width = (coeffs.shape[0] - 1) // 2
    for j in (0, 1):
        cols = jnp.dot(coeffs[...], col_waves[j], precision=highest, preferred_element_type=jnp.float32)
        lane = lax.broadcasted_iota(jnp.int32, (1, TILE), 1)
        if j:
            cols = jnp.where(lane < HALF, -cols, cols)
        for i in (0, 1):
            mixed = jnp.dot(row_waves[i], cols, precision=highest, preferred_element_type=jnp.float32)
            if i:
                place = lax.broadcasted_iota(jnp.int32, (2 * half, 1), 0) % half
                mixed = jnp.where(place < half // 2, -mixed, mixed)
            for part in (0, 1):
                spectrum[part, 2 * j + i] = mixed[part * half : (part + 1) * half]
    count = col_fwd.shape[0]
    none = jnp.zeros((TILE, TILE), jnp.bfloat16)
    for w in range(count):
        first, last = w == 0, w == count - 1
        for third, part in enumerate((0, 0, 1)):
            rows = pl.ds(third * TILE, TILE)
            col_fwd[w, rows, :] = col_base[part]
            if first:
                col_fwd[w, pl.ds(third * TILE + TILE - band_width, band_width), :] = none[:band_width]
            if last:
                col_fwd[w, pl.ds(third * TILE, band_width), :] = none[:band_width]
            inverse = col_base[2 + part].astype(jnp.float32)
            lane = lax.broadcasted_iota(jnp.int32, inverse.shape, 1)
            if not first:
                inverse = jnp.where(lane >= HALF // 2, inverse, 0.0)
            if not last:
                inverse = jnp.where(lane < TILE - HALF // 2, inverse, 0.0)
            col_inv[w, rows, :] = inverse.astype(jnp.bfloat16)


def setup(coeffs, cols):
    band_width = (coeffs.shape[0] - 1) // 2
    windows = cols // HALF - 1
    waves = [jnp.asarray(v) for v in tap_waves(band_width)]
    vmem = pl.BlockSpec(memory_space=pltpu.VMEM)
    return pl.pallas_call(
        setup_kernel,
        out_shape=(
            jax.ShapeDtypeStruct((2, 4, HALF + band_width, TILE), jnp.float32),
            jax.ShapeDtypeStruct((windows, 3 * TILE, TILE), jnp.bfloat16),
            jax.ShapeDtypeStruct((windows, 3 * TILE, TILE), jnp.bfloat16),
        ),
        in_specs=[vmem] * 4,
        out_specs=(vmem,) * 3,
        compiler_params=pltpu.CompilerParams(vmem_limit_bytes=16 * 1024 * 1024),
        name="setup",
    )(coeffs, *waves, jnp.asarray(col_mats()))


def split(value):
    high = value.astype(jnp.bfloat16)
    return high, (value - high.astype(jnp.float32)).astype(jnp.bfloat16)


def dot32(left, right):
    return jnp.dot(left, right, preferred_element_type=jnp.float32)


def replicated_kernel(hx_bits, place, mask, *refs):
    s_near, s_turn, s_far, s_both, r_near, r_turn, r_far, r_both, c_near, c_turn, c_far, c_both = refs[:12]
    spectrum, row_fwd, col_fwd, row_inv, col_inv, out, norms = refs[12:19]
    state, total, w_hi, w_lo, z, y_hi, y_lo, u_hi, u_lo, t_hi, t_lo, wave, left, right = refs[19:]
    rows, cols = state.shape
    col_windows = col_fwd.shape[0]
    half = row_fwd.shape[1]
    quarter = half // 2
    band_width = half - HALF
    tile_rows, tile_cols = rows // TILE, cols // TILE
    block_rows, block_cols = s_near.shape[-2:]
    near_count = s_near.shape[0]
    here_x, here_y, here_c = place[0], place[1], place[2]
    for pos in range(2 * near_count):
        s_row = (here_x ^ hx_bits[0][pos]) * block_rows
        s_row = pl.multiple_of(s_row, block_rows)
        for far, ref in enumerate((s_near, s_far) if pos < near_count else (s_turn, s_both)):
            for k in range(ref.shape[1]):
                s_col = ((here_y ^ k) * 2 + (here_c ^ far)) * block_cols
                s_col = pl.multiple_of(s_col, block_cols)
                value = ref[pos % near_count, k]
                state[pl.ds(s_row, block_rows), pl.ds(s_col, block_cols)] = value
                total[pl.ds(s_row, block_rows), pl.ds(s_col, block_cols)] = value
                high, low = split(value)
                w_hi[pl.ds(s_row, block_rows), pl.ds(s_col, block_cols)] = high
                w_lo[pl.ds(s_row, block_rows), pl.ds(s_col, block_cols)] = low
    share = TILE // block_rows
    for pos in range(2 * near_count):
        index = here_x ^ hx_bits[1][pos]
        a = index // share
        sub = pl.multiple_of((index % share) * block_rows, block_rows)
        for far, ref in enumerate((r_near, r_far) if pos < near_count else (r_turn, r_both)):
            side = here_c ^ far
            for k in range(ref.shape[1]):
                lane = side * (cols // 2) + k * LANES
                b = lane // TILE
                at = pl.multiple_of(lane % TILE, LANES)
                high, low = split(ref[pos % near_count, k] * mask[a, b].astype(jnp.float32))
                for third, part in enumerate((high, high, low)):
                    left[a, b, pl.ds(sub, block_rows), pl.ds(pl.multiple_of(at + third * TILE, LANES), LANES)] = part
    for k in range(2 * c_near.shape[0]):
        for far, ref in enumerate((c_near, c_far) if k < c_near.shape[0] else (c_turn, c_both)):
            lane = ((here_y ^ k) * 2 + (here_c ^ far)) * block_cols
            b = lane // TILE
            at = pl.multiple_of(lane % TILE, block_cols)
            for a in range(tile_rows):
                high, low = split(ref[k % c_near.shape[0], pl.ds(a * TILE, TILE), :])
                for third, part in enumerate((high, high, low)):
                    right[a, b, pl.ds(third * TILE, TILE), pl.ds(at, block_cols)] = part

    for edge in (0, rows + band_width):
        z[pl.ds(edge, band_width), :] = jnp.zeros((band_width, z.shape[1]), jnp.float32)

    def triple(hi_ref, lo_ref, row_at, col_at, axis):
        high = hi_ref[row_at, col_at]
        return jnp.concatenate([high, lo_ref[row_at, col_at], high], axis)

    def step(k, carry):
        keep = jnp.where(k == 0, 0.0, 1.0 - relax_step)
        take = jnp.where(k == 0, 1.0, relax_step)
        every = pl.ds(0, rows)
        for b in range(col_windows):
            at = pl.ds(b * TILE, TILE)
            z[pl.ds(band_width, rows), at] = dot32(triple(w_hi, w_lo, every, pl.ds(b * HALF, TILE), 1), col_fwd[b])
        for a in range(tile_rows):
            for b in range(col_windows):
                cb = pl.ds(b * TILE, TILE)
                upper = z[pl.ds(a * TILE, half), cb]
                lower = z[pl.ds(a * TILE + half, half), cb]
                for part, cells in enumerate((upper + lower, upper - lower)):
                    high, low = split(cells)
                    wave[part] = dot32(row_fwd[part], jnp.concatenate([high, low, high], 0))
                    for i in (0, 1):
                        for j in (0, 1):
                            ri, rj = pl.ds(i * quarter, quarter), pl.ds((1 - i) * quarter, quarter)
                            ci, cj = pl.ds(j * HALF, HALF), pl.ds((1 - j) * HALF, HALF)
                            y = (
                                spectrum[part, 0, ri, ci] * wave[part, ri, ci]
                                + spectrum[part, 1, ri, ci] * wave[part, rj, ci]
                                + spectrum[part, 2, ri, ci] * wave[part, ri, cj]
                                + spectrum[part, 3, ri, ci] * wave[part, rj, cj]
                            )
                            to = pl.ds((2 * a + part) * half + i * quarter, quarter), pl.ds(b * TILE + j * HALF, HALF)
                            y_hi[to], y_lo[to] = split(y)
        for a in range(tile_rows):
            for b in range(col_windows):
                cb = pl.ds(b * TILE, TILE)
                sums, diffs = (
                    dot32(row_inv[part], triple(y_hi, y_lo, pl.ds((2 * a + part) * half, half), cb, 0)) for part in (0, 1)
                )
                upper = sums[band_width:] + diffs[band_width:]
                lower = sums[: half - band_width] - diffs[: half - band_width]
                u_hi[pl.ds(a * TILE, HALF), cb], u_lo[pl.ds(a * TILE, HALF), cb] = split(upper)
                u_hi[pl.ds(a * TILE + HALF, HALF), cb], u_lo[pl.ds(a * TILE + HALF, HALF), cb] = split(lower)
        for a in range(tile_rows):
            for b in range(tile_cols):
                at = pl.ds(a * TILE, TILE), pl.ds(b * TILE, TILE)
                t_hi[at], t_lo[at] = split(dot32(left[a, b], triple(w_hi, w_lo, *at, 0)))
        square = jnp.zeros((8, LANES), jnp.float32)
        for a in range(tile_rows):
            ra = pl.ds(a * TILE, TILE)
            parts = []
            for b in range(col_windows):
                lhs = triple(u_hi, u_lo, ra, pl.ds(b * TILE, TILE), 1)
                rhs = col_inv[b]
                if b % 2 == 0:
                    lhs = jnp.concatenate([lhs, triple(t_hi, t_lo, ra, pl.ds(b // 2 * TILE, TILE), 1)], 1)
                    rhs = jnp.concatenate([rhs, right[a, b // 2]], 0)
                parts.append(dot32(lhs, rhs))
            for j in range(cols // HALF):
                pieces = [parts[b][:, (j - b) * HALF : (j - b + 1) * HALF] for b in range(col_windows) if b <= j <= b + 1]
                cj = pl.ds(j * HALF, HALF)
                residual = keep * state[ra, cj] - take * functools.reduce(jnp.add, pieces)
                state[ra, cj] = residual
                total[ra, cj] = total[ra, cj] + relax_step * residual
                w_hi[ra, cj], w_lo[ra, cj] = split(residual)
                square = square + jnp.sum((residual * residual).reshape(TILE // 8, 8, LANES), 0)
        return jnp.where(norm_lane == k, jnp.sum(square), carry)

    norm_lane = lax.broadcasted_iota(jnp.int32, norms.shape, 1)
    summed = lax.fori_loop(0, ITERS, step, jnp.zeros(norms.shape, jnp.float32))
    norms[...] = jnp.sqrt(summed / (rows * cols) + tiny_square)
    own_row = pl.multiple_of(here_x * block_rows, block_rows)
    own_col = pl.multiple_of((here_y * 2 + here_c) * block_cols, block_cols)
    out[...] = total[pl.ds(own_row, block_rows), pl.ds(own_col, block_cols)]


def swap(value, axis, bit):
    return lax.ppermute(value, axis, [(i, i ^ bit) for i in range(lax.axis_size(axis))])


def doubled(value, axis, bits):
    for bit in bits:
        value = jnp.concatenate([value, swap(value, axis, bit)], 0)
    return value


def bit_places(bits):
    places = [0]
    for bit in bits:
        places = places + [p | bit for p in places]
    return places


def replicated(source, coeffs, row_factor, col_factor, tile_mask):
    block_rows, block_cols = source.shape
    rows, cols = col_factor.shape[0], row_factor.shape[1]
    band_width = (coeffs.shape[0] - 1) // 2
    hx_size, hy_size = lax.axis_size("hx"), lax.axis_size("hy")
    index_x, index_y = lax.axis_index("hx"), lax.axis_index("hy")
    down = [1 << i for i in reversed(range(hx_size.bit_length() - 1))]
    turned = down[:-2] + down[-2:][::-1]
    y_bits = [1 << i for i in range(1, hy_size.bit_length() - 1)]
    s_part = doubled(source[None], "hy", y_bits)
    r_half = lax.dynamic_slice_in_dim(row_factor, (index_y % 2) * (cols // 2), cols // 2, 1)
    r_near = doubled(r_half.reshape(block_rows, -1, LANES).swapaxes(0, 1)[None], "hx", turned[:-1])
    s_near = doubled(s_part[None], "hx", down[:-2])
    s_near = doubled(s_near, "hx", down[-2:-1])
    s_near, coeffs = lax.optimization_barrier((s_near, coeffs))
    ready = setup(coeffs, cols)
    c_near = doubled(col_factor[None], "hy", y_bits[:-1])
    turns = [swap(s_near, "hx", down[-1]), swap(r_near, "hx", turned[-1]), swap(c_near, "hy", y_bits[-1])]
    s_held, *ready = lax.optimization_barrier((s_near, *ready))
    pieces = []
    for near, held, turn in zip((s_near, r_near, c_near), (s_held, r_near, c_near), turns):
        pieces += [near, turn, swap(held, "hy", 1), swap(turn, "hy", 1)]
    spectrum, col_fwd, col_inv = ready
    row_fwd, row_inv = (jnp.asarray(m) for m in row_mats(band_width))
    place = jnp.stack([index_x, index_y // 2, index_y % 2])
    half, col_windows = HALF + band_width, cols // HALF - 1
    vmem = pl.BlockSpec(memory_space=pltpu.VMEM)
    smem = pl.BlockSpec(memory_space=pltpu.SMEM)
    f32, bf16 = jnp.float32, jnp.bfloat16
    tiles = (rows // TILE, cols // TILE)
    shapes = [((rows, cols), f32)] * 2 + [((rows, cols), bf16)] * 2
    shapes += [((rows + 2 * band_width, col_windows * TILE), f32)]
    shapes += [((2 * half * tiles[0], col_windows * TILE), bf16)] * 2 + [((rows, col_windows * TILE), bf16)] * 2
    shapes += [((rows, cols), bf16)] * 2 + [((2, half, TILE), f32)]
    shapes += [(tiles + (TILE, 3 * TILE), bf16), (tiles + (3 * TILE, TILE), bf16)]
    result, norms = pl.pallas_call(
        functools.partial(replicated_kernel, (bit_places(down), bit_places(turned))),
        out_shape=(
            jax.ShapeDtypeStruct((block_rows, block_cols), f32),
            jax.ShapeDtypeStruct((1, ITERS), f32),
        ),
        in_specs=[smem, smem] + [vmem] * 17,
        out_specs=(vmem, vmem),
        scratch_shapes=[pltpu.VMEM(*s) for s in shapes],
        compiler_params=pltpu.CompilerParams(vmem_limit_bytes=50 * 1024 * 1024),
        name="replicated_steps",
    )(place, tile_mask, *pieces, spectrum, row_fwd, col_fwd, row_inv, col_inv)
    return result, norms[0]


def fits(rows, cols, block_rows, block_cols, band_width, hx_size, hy_size):
    powers = all(n & (n - 1) == 0 for n in (hx_size, hy_size))
    whole = rows % TILE == 0 and cols % TILE == 0 and rows > TILE and cols > TILE
    aligned = TILE % block_rows == 0 and block_rows % 16 == 0 and block_cols == LANES and cols % (2 * LANES) == 0
    small = rows * cols * 4 <= GRID_BYTES and 4 * band_width <= TILE and band_width % 32 == 0
    return powers and whole and aligned and small and hx_size >= 4 and hy_size >= 4


def local(source, coeffs, row_factor, col_factor, tile_mask):
    rows, cols = col_factor.shape[0], row_factor.shape[1]
    band_width = (coeffs.shape[0] - 1) // 2
    sizes = lax.axis_size("hx"), lax.axis_size("hy")
    if fits(rows, cols, *source.shape, band_width, *sizes):
        return replicated(source, coeffs, row_factor, col_factor, tile_mask)
    return distributed(source, coeffs, row_factor, col_factor, tile_mask)


def solution(mesh):
    in_specs = (P("hx", "hy"), P(), P("hx", None), P(None, "hy"), P())
    out_specs = (P("hx", "hy"), P())
    return jax.shard_map(local, mesh=mesh, in_specs=in_specs, out_specs=out_specs, check_vma=False)
```

```python
import functools
import jax
import jax.numpy as jnp
import numpy as np
from jax import lax
from jax.experimental import pallas as pl
from jax.experimental.pallas import tpu as pltpu
from jax.sharding import PartitionSpec as P

TILE = 256
ITERS = 8
HALF = TILE // 2
LANES = 128
GRID_BYTES = 2 * 1024 * 1024
LEFT_SCALE, RIGHT_SCALE, VECTOR_SCALE = 16.0, 8.0, 256.0
BACK_SCALE = LEFT_SCALE * RIGHT_SCALE
small = jnp.float8_e5m2


relax_step = 0.25
highest = lax.Precision.HIGHEST
tiny_square = 1e-06


def with_halo(value, sides, width):
    for axis, dim in sides:
        count, length = (lax.axis_size(axis), value.shape[dim])
        up = [(i, (i + 1) % count) for i in range(count - 1)]
        down = [(j, i) for i, j in up]
        last = lax.slice_in_dim(value, length - width, length, axis=dim)
        initial = lax.slice_in_dim(value, 0, width, axis=dim)
        before = lax.ppermute(last, axis, up)
        after = lax.ppermute(initial, axis, down)
        value = jnp.concatenate([before, value, after], axis=dim)
    return value


def swapped(value, axis, apart):
    return lax.ppermute(value, axis, [(i, i ^ 1 << apart) for i in range(lax.axis_size(axis))])


def row_panels(coeffs, row_count, band_width):
    tap_count = 2 * band_width + 1
    padded_rows = row_count + 2 * band_width
    shape_three = (tap_count, row_count, padded_rows)
    tap_index = lax.broadcasted_iota(jnp.int32, shape_three, 0)
    target = lax.broadcasted_iota(jnp.int32, shape_three, 1)
    source_row = lax.broadcasted_iota(jnp.int32, shape_three, 2)
    picker = (source_row == target + 2 * band_width - tap_index).astype(jnp.float32)
    panels = jnp.einsum("pq,pmi->mqi", coeffs, picker, precision=highest)
    return panels.reshape(row_count, tap_count * padded_rows)


def banded_product(field_now, panels, band_width):
    col_count = field_now.shape[1]
    padded = with_halo(field_now, (("hx", 0), ("hy", 1)), band_width)
    pieces = [
        padded[:, 2 * band_width - offset : 2 * band_width - offset + col_count]
        for offset in range(2 * band_width + 1)
    ]
    stacked = jnp.concatenate(pieces, axis=0)
    return jnp.dot(panels, stacked, precision=highest, preferred_element_type=jnp.float32)


def joined(block, partner, upper_half, axis_dim):
    return jnp.where(
        upper_half,
        jnp.concatenate([partner, block], axis_dim),
        jnp.concatenate([block, partner], axis_dim),
    )


def distributed(source, coeffs, row_factor, col_factor, tile_mask):
    row_count, col_count = source.shape
    band_width = (coeffs.shape[0] - 1) // 2
    row_group = TILE // row_count
    col_group = TILE // col_count
    row_index = lax.axis_index("hx")
    col_index = lax.axis_index("hy")
    tile_row = row_index // row_group
    tile_col = col_index // col_group
    panels = row_panels(coeffs, row_count, band_width)
    row_factor_tile = lax.dynamic_slice_in_dim(row_factor, tile_col * TILE, TILE, 1)
    col_factor_tile = lax.dynamic_slice_in_dim(col_factor, tile_row * TILE, TILE, 0)
    mask_rows = lax.broadcasted_iota(jnp.int32, tile_mask.shape, 0)
    mask_cols = lax.broadcasted_iota(jnp.int32, tile_mask.shape, 1)
    chosen = (mask_rows == tile_row) & (mask_cols == tile_col)
    active = jnp.sum(jnp.where(chosen, tile_mask, 0)).astype(jnp.float32)
    solution = source
    squares = []
    for step_index in range(ITERS):
        wide_block = solution
        bit_level = 0
        partner = swapped(wide_block, "hy", bit_level)
        upper_half = col_index // (1 << bit_level) % 2 == 1
        wide_block = joined(wide_block, partner, upper_half, 1)
        mixed_cols = jnp.dot(
            wide_block, col_factor_tile, precision=highest, preferred_element_type=jnp.float32
        )
        tall_block = mixed_cols
        for bit_level in range(row_group.bit_length() - 1):
            partner = swapped(tall_block, "hx", bit_level)
            upper_half = row_index // (1 << bit_level) % 2 == 1
            tall_block = joined(tall_block, partner, upper_half, 0)
        result = jnp.dot(
            row_factor_tile, tall_block, precision=highest, preferred_element_type=jnp.float32
        )
        applied = solution + banded_product(solution, panels, band_width) + active * result
        residual = source - applied
        local_square = jnp.sum(residual * residual)
        squares.append(lax.psum(local_square, ("hx", "hy")))
        solution = solution + relax_step * residual
    summed = jnp.stack(squares)
    cell_count = row_count * col_count * lax.axis_size("hx") * lax.axis_size("hy")
    norm_values = jnp.sqrt(summed / cell_count + tiny_square)
    return (solution, norm_values)


def split_np(value):
    high = value.astype(jnp.bfloat16)
    return high, (value - high.astype(np.float64)).astype(jnp.bfloat16)


def packed_freqs(length):
    half = length // 2
    freq = np.concatenate([np.arange(half), np.arange(half)])
    freq[half] = half
    return freq


def cyclic_mats(length):
    half = length // 2
    phase = 2 * np.pi * ((packed_freqs(length)[:, None] * np.arange(length)[None, :]) % length) / length
    forward = np.concatenate([np.cos(phase[: half + 1]), np.sin(phase[half + 1 :])], 0)
    weight = np.full((length, 1), 2.0 / length)
    weight[0] = weight[half] = 1.0 / length
    return forward, (forward * weight).T


def negacyclic_mats(length):
    half = length // 2
    odd = 2 * np.arange(half) + 1
    phase = 2 * np.pi * ((odd[:, None] * np.arange(length)[None, :]) % (2 * length)) / (2 * length)
    forward = np.concatenate([np.cos(phase), np.sin(phase)], 0)
    return forward, (forward * (2.0 / length)).T


def row_mats(band_width):
    half = (TILE + 2 * band_width) // 2
    fwd, inv = [], []
    for forward, inverse in (cyclic_mats(half), negacyclic_mats(half)):
        fh, fl = split_np(forward)
        gh, gl = split_np(inverse * 0.5)
        fwd.append(np.concatenate([fh, fh, fl], 1))
        inv.append(np.concatenate([gh, gh, gl], 1))
    return np.stack(fwd), np.stack(inv)


def col_mats():
    forward, inverse = cyclic_mats(TILE)
    return np.stack(split_np(forward.T) + split_np(inverse.T * BACK_SCALE))


def tap_waves(band_width):
    offset = np.arange(-band_width, band_width + 1)
    half = (TILE + 2 * band_width) // 2
    odd = 2 * np.arange(half // 2) + 1
    row_freq = np.concatenate([2 * packed_freqs(half), odd, odd])
    row_phase = 2 * np.pi * ((row_freq[:, None] * offset[None, :]) % (2 * half)) / (2 * half)
    col_phase = 2 * np.pi * ((packed_freqs(TILE)[:, None] * offset[None, :]) % TILE) / TILE
    rows = np.stack([np.cos(row_phase), np.sin(row_phase)]).astype(np.float32)
    cols = np.stack([np.cos(col_phase).T, np.sin(col_phase).T]).astype(np.float32)
    return rows, cols


def setup_kernel(coeffs, row_waves, col_waves, col_base, spectrum, col_main, col_small):
    half = spectrum.shape[2]
    band_width = (coeffs.shape[0] - 1) // 2
    for j in (0, 1):
        cols = jnp.dot(coeffs[...], col_waves[j], precision=highest, preferred_element_type=jnp.float32)
        lane = lax.broadcasted_iota(jnp.int32, (1, TILE), 1)
        if j:
            cols = jnp.where(lane < HALF, -cols, cols)
        for i in (0, 1):
            mixed = jnp.dot(row_waves[i], cols, precision=highest, preferred_element_type=jnp.float32)
            if i:
                place = lax.broadcasted_iota(jnp.int32, (2 * half, 1), 0) % half
                mixed = jnp.where(place < half // 2, -mixed, mixed)
            for part in (0, 1):
                spectrum[part, 2 * j + i] = mixed[part * half : (part + 1) * half]
    count = col_main.shape[1]
    for w in range(count):
        for way in (0, 1):
            for part in (0, 1):
                cells = col_base[2 * way + part].astype(jnp.float32)
                place = lax.broadcasted_iota(jnp.int32, cells.shape, way)
                margin = HALF // 2 if way else band_width
                if (w > 0) if way else (w == count - 1):
                    cells = jnp.where(place >= margin, cells, 0.0)
                if (w < count - 1) if way else (w == 0):
                    cells = jnp.where(place < TILE - margin, cells, 0.0)
                if part == 0:
                    col_main[way, w] = cells.astype(jnp.bfloat16)
                col_small[way, w, part * TILE : (part + 1) * TILE] = cells.astype(small)


def setup(coeffs, cols):
    band_width = (coeffs.shape[0] - 1) // 2
    windows = cols // HALF - 1
    waves = [jnp.asarray(v) for v in tap_waves(band_width)]
    vmem = pl.BlockSpec(memory_space=pltpu.VMEM)
    return pl.pallas_call(
        setup_kernel,
        out_shape=(
            jax.ShapeDtypeStruct((2, 4, HALF + band_width, TILE), jnp.float32),
            jax.ShapeDtypeStruct((2, windows, TILE, TILE), jnp.bfloat16),
            jax.ShapeDtypeStruct((2, windows, 2 * TILE, TILE), small),
        ),
        in_specs=[vmem] * 4,
        out_specs=(vmem,) * 3,
        compiler_params=pltpu.CompilerParams(vmem_limit_bytes=16 * 1024 * 1024),
        name="setup",
    )(coeffs, *waves, jnp.asarray(col_mats()))


def split(value):
    high = value.astype(jnp.bfloat16)
    return high, (value - high.astype(jnp.float32)).astype(jnp.bfloat16)


def split_small(value):
    high = value.astype(jnp.bfloat16)
    low = (value - high.astype(jnp.float32)).astype(jnp.bfloat16)
    most = jnp.asarray(jnp.finfo(small).max, jnp.bfloat16)
    return high, jnp.clip(low, -most, most).astype(small), jnp.clip(high, -most, most).astype(small)


def dot32(left, right):
    return jnp.dot(left, right, preferred_element_type=jnp.float32)


def replicated_kernel(hx_bits, place, mask, *refs):
    s_near, s_turn, s_far, s_both, r_near, r_turn, r_far, r_both, c_near, c_turn, c_far, c_both = refs[:12]
    spectrum, row_fwd, row_inv, col_main, col_small, out, norms = refs[12:19]
    state, total, z, y_hi, y_lo, w_main, w_rest, w_same, u_main, u_rest, u_same, t_main, t_rest, t_same = refs[19:33]
    left_main, left_small, right_main, right_small, scale = refs[33:]
    w, u, t = (w_main, w_rest, w_same), (u_main, u_rest, u_same), (t_main, t_rest, t_same)
    rows, cols = state.shape
    col_windows = col_main.shape[1]
    half = row_fwd.shape[1]
    quarter = half // 2
    band_width = half - HALF
    tile_rows, tile_cols = rows // TILE, cols // TILE
    block_rows, block_cols = s_near.shape[-2:]
    near_count = s_near.shape[0]
    here_x, here_y, here_c = place[0], place[1], place[2]
    square = jnp.zeros((8, LANES), jnp.float32)
    for pos in range(2 * near_count):
        s_row = (here_x ^ hx_bits[0][pos]) * block_rows
        s_row = pl.multiple_of(s_row, block_rows)
        for far, ref in enumerate((s_near, s_far) if pos < near_count else (s_turn, s_both)):
            for k in range(ref.shape[1]):
                s_col = ((here_y ^ k) * 2 + (here_c ^ far)) * block_cols
                s_col = pl.multiple_of(s_col, block_cols)
                value = ref[pos % near_count, k]
                state[pl.ds(s_row, block_rows), pl.ds(s_col, block_cols)] = value
                total[pl.ds(s_row, block_rows), pl.ds(s_col, block_cols)] = value
                square = square + jnp.sum((value * value).reshape(block_rows // 8, 8, block_cols), 0)
    share = TILE // block_rows
    for pos in range(2 * near_count):
        index = here_x ^ hx_bits[1][pos]
        a = index // share
        sub = pl.multiple_of((index % share) * block_rows, block_rows)
        for far, ref in enumerate((r_near, r_far) if pos < near_count else (r_turn, r_both)):
            side = here_c ^ far
            for k in range(ref.shape[1]):
                lane = side * (cols // 2) + k * LANES
                b = lane // TILE
                at = pl.multiple_of(lane % TILE, LANES)
                cells = ref[pos % near_count, k] * (LEFT_SCALE * mask[a, b].astype(jnp.float32))
                high, rest, same = split_small(cells)
                left_main[a, b, pl.ds(sub, block_rows), pl.ds(at, LANES)] = high
                left_small[a, b, pl.ds(sub, block_rows), pl.ds(at, LANES)] = same
                left_small[a, b, pl.ds(sub, block_rows), pl.ds(pl.multiple_of(at + TILE, LANES), LANES)] = rest
    for k in range(2 * c_near.shape[0]):
        for far, ref in enumerate((c_near, c_far) if k < c_near.shape[0] else (c_turn, c_both)):
            lane = ((here_y ^ k) * 2 + (here_c ^ far)) * block_cols
            b = lane // TILE
            at = pl.multiple_of(lane % TILE, block_cols)
            for a in range(tile_rows):
                high, rest, same = split_small(ref[k % c_near.shape[0], pl.ds(a * TILE, TILE), :] * RIGHT_SCALE)
                right_main[a, b, :, pl.ds(at, block_cols)] = high
                right_small[a, b, pl.ds(0, TILE), pl.ds(at, block_cols)] = same
                right_small[a, b, pl.ds(TILE, TILE), pl.ds(at, block_cols)] = rest

    for edge in (0, rows + band_width):
        z[pl.ds(edge, band_width), :] = jnp.zeros((band_width, z.shape[1]), jnp.float32)

    def triple(hi_ref, lo_ref, row_at, col_at, axis):
        high = hi_ref[row_at, col_at]
        return jnp.concatenate([high, lo_ref[row_at, col_at], high], axis)

    def put(refs, at, value):
        for ref, part in zip(refs, split_small(value)):
            ref[at] = part

    def scaled_by(sum_square):
        return VECTOR_SCALE * lax.rsqrt(jnp.maximum(jnp.full((8, LANES), sum_square), 1e-30))

    def times(cells, factor):
        return (cells.reshape(-1, 8, LANES) * factor).reshape(cells.shape)

    def columns(b):
        at = slice(None), pl.ds(b * HALF, TILE)
        rest_same = jnp.concatenate([w_rest[at], w_same[at]], 1)
        z[pl.ds(band_width, rows), pl.ds(b * TILE, TILE)] = dot32(w_main[at], col_main[0, b]) + dot32(
            rest_same, col_small[0, b]
        )

    def spectral(a, b, part):
        cb = pl.ds(b * TILE, TILE)
        upper = z[pl.ds(a * TILE, half), cb]
        lower = z[pl.ds(a * TILE + half, half), cb]
        high, low = split(upper - lower if part else upper + lower)
        wave = dot32(row_fwd[part], jnp.concatenate([high, low, high], 0))
        for i in (0, 1):
            for j in (0, 1):
                ri, rj = slice(i * quarter, (i + 1) * quarter), slice((1 - i) * quarter, (2 - i) * quarter)
                ci, cj = slice(j * HALF, (j + 1) * HALF), slice((1 - j) * HALF, (2 - j) * HALF)
                y = (
                    spectrum[part, 0, ri, ci] * wave[ri, ci]
                    + spectrum[part, 1, ri, ci] * wave[rj, ci]
                    + spectrum[part, 2, ri, ci] * wave[ri, cj]
                    + spectrum[part, 3, ri, ci] * wave[rj, cj]
                )
                to = pl.ds((2 * a + part) * half + i * quarter, quarter), pl.ds(b * TILE + j * HALF, HALF)
                y_hi[to], y_lo[to] = split(y)

    def back_rows(a, b):
        cb = pl.ds(b * TILE, TILE)
        sums, diffs = (
            dot32(row_inv[part], triple(y_hi, y_lo, pl.ds((2 * a + part) * half, half), cb, 0)) for part in (0, 1)
        )
        upper = sums[band_width:] + diffs[band_width:]
        lower = sums[: half - band_width] - diffs[: half - band_width]
        put(u, (pl.ds(a * TILE, HALF), cb), upper)
        put(u, (pl.ds(a * TILE + HALF, HALF), cb), lower)

    def tile_left(a, b):
        at = pl.ds(a * TILE, TILE), pl.ds(b * TILE, TILE)
        rest_same = jnp.concatenate([w_rest[at], w_same[at]], 0)
        put(t, at, dot32(left_main[a, b], w_main[at]) + dot32(left_small[a, b], rest_same))

    def update(a, keep, take, factor):
        ra = pl.ds(a * TILE, TILE)
        square = jnp.zeros((8, LANES), jnp.float32)
        parts = []
        for b in range(col_windows):
            at = ra, pl.ds(b * TILE, TILE)
            lhs, lhs_small, rhs, rhs_small = [u_main[at]], [u_rest[at], u_same[at]], [col_main[1, b]], [col_small[1, b]]
            if b % 2 == 0:
                at = ra, pl.ds(b // 2 * TILE, TILE)
                lhs, lhs_small = lhs + [t_main[at]], lhs_small + [t_rest[at], t_same[at]]
                rhs, rhs_small = rhs + [right_main[a, b // 2]], rhs_small + [right_small[a, b // 2]]
            parts.append(
                dot32(jnp.concatenate(lhs, 1), jnp.concatenate(rhs, 0))
                + dot32(jnp.concatenate(lhs_small, 1), jnp.concatenate(rhs_small, 0))
            )
        for j in range(cols // HALF):
            pieces = [parts[b][:, (j - b) * HALF : (j - b + 1) * HALF] for b in range(col_windows) if b <= j <= b + 1]
            cj = pl.ds(j * HALF, HALF)
            residual = keep * state[ra, cj] - times(functools.reduce(jnp.add, pieces), take)
            state[ra, cj] = residual
            total[ra, cj] = total[ra, cj] + relax_step * residual
            put(w, (ra, cj), times(residual, factor))
            square = square + jnp.sum((residual * residual).reshape(TILE // 8, 8, LANES), 0)
        return square

    def step(k, carry):
        sums, last = carry
        keep = jnp.where(k == 0, 0.0, 1.0 - relax_step)
        take = jnp.where(k == 0, 1.0, relax_step) / (BACK_SCALE * scale[...])
        factor = scaled_by(last)
        tiles = [(a, b) for a in range(tile_rows) for b in range(tile_cols)]
        for b in range(col_windows):
            columns(b)
        for b in range(col_windows):
            for a in range(tile_rows):
                spectral(a, b, 0)
                spectral(a, b, 1)
                if tiles:
                    tile_left(*tiles.pop(0))
                if b:
                    back_rows(a, b - 1)
        for at in tiles:
            tile_left(*at)
        for a in range(tile_rows):
            back_rows(a, col_windows - 1)
        square = jnp.zeros((8, LANES), jnp.float32)
        for a in range(tile_rows):
            square = square + update(a, keep, take, factor)
        scale[...] = factor
        sum_square = jnp.sum(square)
        return jnp.where(norm_lane == k, sum_square, sums), sum_square

    sum_square = jnp.sum(square)
    scale[...] = scaled_by(sum_square)
    for i in range(0, rows, TILE):
        for j in range(0, cols, LANES):
            at = pl.ds(i, TILE), pl.ds(j, LANES)
            put(w, at, times(state[at], scale[...]))
    norm_lane = lax.broadcasted_iota(jnp.int32, norms.shape, 1)
    summed, _ = lax.fori_loop(0, ITERS, step, (jnp.zeros(norms.shape, jnp.float32), sum_square))
    norms[...] = jnp.sqrt(summed / (rows * cols) + tiny_square)
    own_row = pl.multiple_of(here_x * block_rows, block_rows)
    own_col = pl.multiple_of((here_y * 2 + here_c) * block_cols, block_cols)
    out[...] = total[pl.ds(own_row, block_rows), pl.ds(own_col, block_cols)]


def swap(value, axis, bit):
    return lax.ppermute(value, axis, [(i, i ^ bit) for i in range(lax.axis_size(axis))])


def doubled(value, axis, bits):
    for bit in bits:
        value = jnp.concatenate([value, swap(value, axis, bit)], 0)
    return value


def bit_places(bits):
    places = [0]
    for bit in bits:
        places = places + [p | bit for p in places]
    return places


def replicated(source, coeffs, row_factor, col_factor, tile_mask):
    block_rows, block_cols = source.shape
    rows, cols = col_factor.shape[0], row_factor.shape[1]
    band_width = (coeffs.shape[0] - 1) // 2
    hx_size, hy_size = lax.axis_size("hx"), lax.axis_size("hy")
    index_x, index_y = lax.axis_index("hx"), lax.axis_index("hy")
    down = [1 << i for i in reversed(range(hx_size.bit_length() - 1))]
    turned = down[:-2] + down[-2:][::-1]
    y_bits = [1 << i for i in range(1, hy_size.bit_length() - 1)]
    s_part = doubled(source[None], "hy", y_bits)
    r_half = lax.dynamic_slice_in_dim(row_factor, (index_y % 2) * (cols // 2), cols // 2, 1)
    r_near = doubled(r_half.reshape(block_rows, -1, LANES).swapaxes(0, 1)[None], "hx", turned[:-1])
    s_near = doubled(s_part[None], "hx", down[:-2])
    s_near = doubled(s_near, "hx", down[-2:-1])
    s_near, coeffs = lax.optimization_barrier((s_near, coeffs))
    ready = setup(coeffs, cols)
    c_near = doubled(col_factor[None], "hy", y_bits[:-1])
    turns = [swap(s_near, "hx", down[-1]), swap(r_near, "hx", turned[-1]), swap(c_near, "hy", y_bits[-1])]
    s_held, *ready = lax.optimization_barrier((s_near, *ready))
    pieces = []
    for near, held, turn in zip((s_near, r_near, c_near), (s_held, r_near, c_near), turns):
        pieces += [near, turn, swap(held, "hy", 1), swap(turn, "hy", 1)]
    spectrum, col_main, col_small = ready
    row_fwd, row_inv = (jnp.asarray(m) for m in row_mats(band_width))
    place = jnp.stack([index_x, index_y // 2, index_y % 2])
    half, col_windows = HALF + band_width, cols // HALF - 1
    vmem = pl.BlockSpec(memory_space=pltpu.VMEM)
    smem = pl.BlockSpec(memory_space=pltpu.SMEM)
    f32, bf16 = jnp.float32, jnp.bfloat16
    tiles = (rows // TILE, cols // TILE)
    wide = col_windows * TILE
    shapes = [((rows, cols), f32)] * 2 + [((rows + 2 * band_width, wide), f32)]
    shapes += [((2 * half * tiles[0], wide), bf16)] * 2
    for shape in ((rows, cols), (rows, wide), (rows, cols)):
        shapes += [(shape, bf16), (shape, small), (shape, small)]
    shapes += [(tiles + (TILE, TILE), bf16), (tiles + (TILE, 2 * TILE), small)]
    shapes += [(tiles + (TILE, TILE), bf16), (tiles + (2 * TILE, TILE), small), ((8, LANES), f32)]
    result, norms = pl.pallas_call(
        functools.partial(replicated_kernel, (bit_places(down), bit_places(turned))),
        out_shape=(
            jax.ShapeDtypeStruct((block_rows, block_cols), f32),
            jax.ShapeDtypeStruct((1, ITERS), f32),
        ),
        in_specs=[smem, smem] + [vmem] * 17,
        out_specs=(vmem, vmem),
        scratch_shapes=[pltpu.VMEM(*s) for s in shapes],
        compiler_params=pltpu.CompilerParams(vmem_limit_bytes=50 * 1024 * 1024),
        name="replicated_steps",
    )(place, tile_mask, *pieces, spectrum, row_fwd, row_inv, col_main, col_small)
    return result, norms[0]


def fits(rows, cols, block_rows, block_cols, band_width, hx_size, hy_size):
    powers = all(n & (n - 1) == 0 for n in (hx_size, hy_size))
    whole = rows % TILE == 0 and cols % TILE == 0 and rows > TILE and cols > TILE
    aligned = TILE % block_rows == 0 and block_rows % 16 == 0 and block_cols == LANES and cols % (2 * LANES) == 0
    small = rows * cols * 4 <= GRID_BYTES and 4 * band_width <= TILE and band_width % 32 == 0
    return powers and whole and aligned and small and hx_size >= 4 and hy_size >= 4


def local(source, coeffs, row_factor, col_factor, tile_mask):
    rows, cols = col_factor.shape[0], row_factor.shape[1]
    band_width = (coeffs.shape[0] - 1) // 2
    sizes = lax.axis_size("hx"), lax.axis_size("hy")
    if fits(rows, cols, *source.shape, band_width, *sizes):
        return replicated(source, coeffs, row_factor, col_factor, tile_mask)
    return distributed(source, coeffs, row_factor, col_factor, tile_mask)


def solution(mesh):
    in_specs = (P("hx", "hy"), P(), P("hx", None), P(None, "hy"), P())
    out_specs = (P("hx", "hy"), P())
    return jax.shard_map(local, mesh=mesh, in_specs=in_specs, out_specs=out_specs, check_vma=False)
```

```python
import functools
import jax
import jax.numpy as jnp
import numpy as np
from jax import lax
from jax.experimental import pallas as pl
from jax.experimental.pallas import tpu as pltpu
from jax.sharding import PartitionSpec as P

TILE = 256
ITERS = 8
HALF = TILE // 2
LANES = 128
GRID_BYTES = 2 * 1024 * 1024
LEFT_SCALE, RIGHT_SCALE, VECTOR_SCALE = 16.0, 8.0, 256.0
BACK_SCALE = LEFT_SCALE * RIGHT_SCALE
small = jnp.float8_e5m2


relax_step = 0.25
highest = lax.Precision.HIGHEST
tiny_square = 1e-06


def with_halo(value, sides, width):
    for axis, dim in sides:
        count, length = (lax.axis_size(axis), value.shape[dim])
        up = [(i, (i + 1) % count) for i in range(count - 1)]
        down = [(j, i) for i, j in up]
        last = lax.slice_in_dim(value, length - width, length, axis=dim)
        initial = lax.slice_in_dim(value, 0, width, axis=dim)
        before = lax.ppermute(last, axis, up)
        after = lax.ppermute(initial, axis, down)
        value = jnp.concatenate([before, value, after], axis=dim)
    return value


def swapped(value, axis, apart):
    return lax.ppermute(value, axis, [(i, i ^ 1 << apart) for i in range(lax.axis_size(axis))])


def row_panels(coeffs, row_count, band_width):
    tap_count = 2 * band_width + 1
    padded_rows = row_count + 2 * band_width
    shape_three = (tap_count, row_count, padded_rows)
    tap_index = lax.broadcasted_iota(jnp.int32, shape_three, 0)
    target = lax.broadcasted_iota(jnp.int32, shape_three, 1)
    source_row = lax.broadcasted_iota(jnp.int32, shape_three, 2)
    picker = (source_row == target + 2 * band_width - tap_index).astype(jnp.float32)
    panels = jnp.einsum("pq,pmi->mqi", coeffs, picker, precision=highest)
    return panels.reshape(row_count, tap_count * padded_rows)


def banded_product(field_now, panels, band_width):
    col_count = field_now.shape[1]
    padded = with_halo(field_now, (("hx", 0), ("hy", 1)), band_width)
    pieces = [
        padded[:, 2 * band_width - offset : 2 * band_width - offset + col_count]
        for offset in range(2 * band_width + 1)
    ]
    stacked = jnp.concatenate(pieces, axis=0)
    return jnp.dot(panels, stacked, precision=highest, preferred_element_type=jnp.float32)


def joined(block, partner, upper_half, axis_dim):
    return jnp.where(
        upper_half,
        jnp.concatenate([partner, block], axis_dim),
        jnp.concatenate([block, partner], axis_dim),
    )


def distributed(source, coeffs, row_factor, col_factor, tile_mask):
    row_count, col_count = source.shape
    band_width = (coeffs.shape[0] - 1) // 2
    row_group = TILE // row_count
    col_group = TILE // col_count
    row_index = lax.axis_index("hx")
    col_index = lax.axis_index("hy")
    tile_row = row_index // row_group
    tile_col = col_index // col_group
    panels = row_panels(coeffs, row_count, band_width)
    row_factor_tile = lax.dynamic_slice_in_dim(row_factor, tile_col * TILE, TILE, 1)
    col_factor_tile = lax.dynamic_slice_in_dim(col_factor, tile_row * TILE, TILE, 0)
    mask_rows = lax.broadcasted_iota(jnp.int32, tile_mask.shape, 0)
    mask_cols = lax.broadcasted_iota(jnp.int32, tile_mask.shape, 1)
    chosen = (mask_rows == tile_row) & (mask_cols == tile_col)
    active = jnp.sum(jnp.where(chosen, tile_mask, 0)).astype(jnp.float32)
    solution = source
    squares = []
    for step_index in range(ITERS):
        wide_block = solution
        bit_level = 0
        partner = swapped(wide_block, "hy", bit_level)
        upper_half = col_index // (1 << bit_level) % 2 == 1
        wide_block = joined(wide_block, partner, upper_half, 1)
        mixed_cols = jnp.dot(
            wide_block, col_factor_tile, precision=highest, preferred_element_type=jnp.float32
        )
        tall_block = mixed_cols
        for bit_level in range(row_group.bit_length() - 1):
            partner = swapped(tall_block, "hx", bit_level)
            upper_half = row_index // (1 << bit_level) % 2 == 1
            tall_block = joined(tall_block, partner, upper_half, 0)
        result = jnp.dot(
            row_factor_tile, tall_block, precision=highest, preferred_element_type=jnp.float32
        )
        applied = solution + banded_product(solution, panels, band_width) + active * result
        residual = source - applied
        local_square = jnp.sum(residual * residual)
        squares.append(lax.psum(local_square, ("hx", "hy")))
        solution = solution + relax_step * residual
    summed = jnp.stack(squares)
    cell_count = row_count * col_count * lax.axis_size("hx") * lax.axis_size("hy")
    norm_values = jnp.sqrt(summed / cell_count + tiny_square)
    return (solution, norm_values)


def split_np(value):
    high = value.astype(jnp.bfloat16)
    return high, (value - high.astype(np.float64)).astype(jnp.bfloat16)


def packed_freqs(length):
    half = length // 2
    freq = np.concatenate([np.arange(half), np.arange(half)])
    freq[half] = half
    return freq


def cyclic_mats(length):
    half = length // 2
    phase = 2 * np.pi * ((packed_freqs(length)[:, None] * np.arange(length)[None, :]) % length) / length
    forward = np.concatenate([np.cos(phase[: half + 1]), np.sin(phase[half + 1 :])], 0)
    weight = np.full((length, 1), 2.0 / length)
    weight[0] = weight[half] = 1.0 / length
    return forward, (forward * weight).T


def negacyclic_mats(length):
    half = length // 2
    odd = 2 * np.arange(half) + 1
    phase = 2 * np.pi * ((odd[:, None] * np.arange(length)[None, :]) % (2 * length)) / (2 * length)
    forward = np.concatenate([np.cos(phase), np.sin(phase)], 0)
    return forward, (forward * (2.0 / length)).T


def row_mats(band_width):
    half = (TILE + 2 * band_width) // 2
    fwd, inv = [], []
    for forward, inverse in (cyclic_mats(half), negacyclic_mats(half)):
        fh, fl = split_np(forward)
        gh, gl = split_np(inverse * 0.5)
        fwd.append(np.concatenate([fh, fh, fl], 1))
        inv.append(np.concatenate([gh, gh, gl], 1))
    return np.stack(fwd), np.stack(inv)


def col_mats():
    forward, inverse = cyclic_mats(TILE)
    return np.stack(split_np(forward.T) + split_np(inverse.T * BACK_SCALE))


def tap_waves(band_width):
    offset = np.arange(-band_width, band_width + 1)
    half = (TILE + 2 * band_width) // 2
    odd = 2 * np.arange(half // 2) + 1
    row_freq = np.concatenate([2 * packed_freqs(half), odd, odd])
    row_phase = 2 * np.pi * ((row_freq[:, None] * offset[None, :]) % (2 * half)) / (2 * half)
    col_phase = 2 * np.pi * ((packed_freqs(TILE)[:, None] * offset[None, :]) % TILE) / TILE
    rows = np.stack([np.cos(row_phase), np.sin(row_phase)]).astype(np.float32)
    cols = np.stack([np.cos(col_phase).T, np.sin(col_phase).T]).astype(np.float32)
    return rows, cols


def setup_kernel(coeffs, row_waves, col_waves, col_base, spectrum, col_main, col_small):
    half = spectrum.shape[2]
    band_width = (coeffs.shape[0] - 1) // 2
    for j in (0, 1):
        cols = jnp.dot(coeffs[...], col_waves[j], precision=highest, preferred_element_type=jnp.float32)
        lane = lax.broadcasted_iota(jnp.int32, (1, TILE), 1)
        if j:
            cols = jnp.where(lane < HALF, -cols, cols)
        for i in (0, 1):
            mixed = jnp.dot(row_waves[i], cols, precision=highest, preferred_element_type=jnp.float32)
            if i:
                place = lax.broadcasted_iota(jnp.int32, (2 * half, 1), 0) % half
                mixed = jnp.where(place < half // 2, -mixed, mixed)
            for part in (0, 1):
                spectrum[part, 2 * j + i] = mixed[part * half : (part + 1) * half]
    count = col_main.shape[1]
    for w in range(count):
        for way in (0, 1):
            for part in (0, 1):
                cells = col_base[2 * way + part].astype(jnp.float32)
                place = lax.broadcasted_iota(jnp.int32, cells.shape, way)
                margin = HALF // 2 if way else band_width
                if (w > 0) if way else (w == count - 1):
                    cells = jnp.where(place >= margin, cells, 0.0)
                if (w < count - 1) if way else (w == 0):
                    cells = jnp.where(place < TILE - margin, cells, 0.0)
                if part == 0:
                    col_main[way, w] = cells.astype(jnp.bfloat16)
                col_small[way, w, part * TILE : (part + 1) * TILE] = cells.astype(small)


def setup(coeffs, cols):
    band_width = (coeffs.shape[0] - 1) // 2
    windows = cols // HALF - 1
    waves = [jnp.asarray(v) for v in tap_waves(band_width)]
    vmem = pl.BlockSpec(memory_space=pltpu.VMEM)
    return pl.pallas_call(
        setup_kernel,
        out_shape=(
            jax.ShapeDtypeStruct((2, 4, HALF + band_width, TILE), jnp.float32),
            jax.ShapeDtypeStruct((2, windows, TILE, TILE), jnp.bfloat16),
            jax.ShapeDtypeStruct((2, windows, 2 * TILE, TILE), small),
        ),
        in_specs=[vmem] * 4,
        out_specs=(vmem,) * 3,
        compiler_params=pltpu.CompilerParams(vmem_limit_bytes=16 * 1024 * 1024),
        name="setup",
    )(coeffs, *waves, jnp.asarray(col_mats()))


def split(value):
    high = value.astype(jnp.bfloat16)
    return high, (value - high.astype(jnp.float32)).astype(jnp.bfloat16)


def split_small(value):
    high = value.astype(jnp.bfloat16)
    low = (value - high.astype(jnp.float32)).astype(jnp.bfloat16)
    most = jnp.asarray(jnp.finfo(small).max, jnp.bfloat16)
    return high, jnp.clip(low, -most, most).astype(small), jnp.clip(high, -most, most).astype(small)


def dot32(left, right):
    return jnp.dot(left, right, preferred_element_type=jnp.float32)


def replicated_kernel(hx_bits, place, mask, *refs):
    sources, (out, norms), held = refs[:17], refs[17:19], refs[38:55]
    loads = [pltpu.make_async_copy(a, b, refs[55].at[i]) for i, (a, b) in enumerate(zip(sources, held))]
    for load in loads:
        load.start()
    s_near, s_turn, s_far, s_both, r_near, r_turn, r_far, r_both, c_near, c_turn, c_far, c_both = held[:12]
    spectrum, row_fwd, row_inv, col_main, col_small = held[12:]
    state, total, z, y_hi, y_lo, w_main, w_rest, w_same, u_main, u_rest, u_same, t_main, t_rest, t_same = refs[19:33]
    left_main, left_small, right_main, right_small, scale = refs[33:38]
    w, u, t = (w_main, w_rest, w_same), (u_main, u_rest, u_same), (t_main, t_rest, t_same)
    rows, cols = state.shape
    col_windows = col_main.shape[1]
    half = row_fwd.shape[1]
    quarter = half // 2
    band_width = half - HALF
    tile_rows, tile_cols = rows // TILE, cols // TILE
    block_rows, block_cols = s_near.shape[-2:]
    near_count = s_near.shape[0]
    here_x, here_y, here_c = place[0], place[1], place[2]
    square = jnp.zeros((8, LANES), jnp.float32)
    for load in loads[:4]:
        load.wait()
    for pos in range(2 * near_count):
        s_row = (here_x ^ hx_bits[0][pos]) * block_rows
        s_row = pl.multiple_of(s_row, block_rows)
        for far, ref in enumerate((s_near, s_far) if pos < near_count else (s_turn, s_both)):
            for k in range(ref.shape[1]):
                s_col = ((here_y ^ k) * 2 + (here_c ^ far)) * block_cols
                s_col = pl.multiple_of(s_col, block_cols)
                value = ref[pos % near_count, k]
                state[pl.ds(s_row, block_rows), pl.ds(s_col, block_cols)] = value
                total[pl.ds(s_row, block_rows), pl.ds(s_col, block_cols)] = value
                square = square + jnp.sum((value * value).reshape(block_rows // 8, 8, block_cols), 0)
    for load in loads[4:8]:
        load.wait()
    share = TILE // block_rows
    for pos in range(2 * near_count):
        index = here_x ^ hx_bits[1][pos]
        a = index // share
        sub = pl.multiple_of((index % share) * block_rows, block_rows)
        for far, ref in enumerate((r_near, r_far) if pos < near_count else (r_turn, r_both)):
            side = here_c ^ far
            for k in range(ref.shape[1]):
                lane = side * (cols // 2) + k * LANES
                b = lane // TILE
                at = pl.multiple_of(lane % TILE, LANES)
                cells = ref[pos % near_count, k] * (LEFT_SCALE * mask[a, b].astype(jnp.float32))
                high, rest, same = split_small(cells)
                left_main[a, b, pl.ds(sub, block_rows), pl.ds(at, LANES)] = high
                left_small[a, b, pl.ds(sub, block_rows), pl.ds(at, LANES)] = same
                left_small[a, b, pl.ds(sub, block_rows), pl.ds(pl.multiple_of(at + TILE, LANES), LANES)] = rest
    for load in loads[8:12]:
        load.wait()
    for k in range(2 * c_near.shape[0]):
        for far, ref in enumerate((c_near, c_far) if k < c_near.shape[0] else (c_turn, c_both)):
            lane = ((here_y ^ k) * 2 + (here_c ^ far)) * block_cols
            b = lane // TILE
            at = pl.multiple_of(lane % TILE, block_cols)
            for a in range(tile_rows):
                high, rest, same = split_small(ref[k % c_near.shape[0], pl.ds(a * TILE, TILE), :] * RIGHT_SCALE)
                right_main[a, b, :, pl.ds(at, block_cols)] = high
                right_small[a, b, pl.ds(0, TILE), pl.ds(at, block_cols)] = same
                right_small[a, b, pl.ds(TILE, TILE), pl.ds(at, block_cols)] = rest

    for edge in (0, rows + band_width):
        z[pl.ds(edge, band_width), :] = jnp.zeros((band_width, z.shape[1]), jnp.float32)

    def triple(hi_ref, lo_ref, row_at, col_at, axis):
        high = hi_ref[row_at, col_at]
        return jnp.concatenate([high, lo_ref[row_at, col_at], high], axis)

    def put(refs, at, value):
        for ref, part in zip(refs, split_small(value)):
            ref[at] = part

    def scaled_by(sum_square):
        return VECTOR_SCALE * lax.rsqrt(jnp.maximum(jnp.full((8, LANES), sum_square), 1e-30))

    def times(cells, factor):
        return (cells.reshape(-1, 8, LANES) * factor).reshape(cells.shape)

    def columns(b):
        at = slice(None), pl.ds(b * HALF, TILE)
        rest_same = jnp.concatenate([w_rest[at], w_same[at]], 1)
        z[pl.ds(band_width, rows), pl.ds(b * TILE, TILE)] = dot32(w_main[at], col_main[0, b]) + dot32(
            rest_same, col_small[0, b]
        )

    def spectral(a, b, part):
        cb = pl.ds(b * TILE, TILE)
        upper = z[pl.ds(a * TILE, half), cb]
        lower = z[pl.ds(a * TILE + half, half), cb]
        high, low = split(upper - lower if part else upper + lower)
        wave = dot32(row_fwd[part], jnp.concatenate([high, low, high], 0))
        for i in (0, 1):
            for j in (0, 1):
                ri, rj = slice(i * quarter, (i + 1) * quarter), slice((1 - i) * quarter, (2 - i) * quarter)
                ci, cj = slice(j * HALF, (j + 1) * HALF), slice((1 - j) * HALF, (2 - j) * HALF)
                y = (
                    spectrum[part, 0, ri, ci] * wave[ri, ci]
                    + spectrum[part, 1, ri, ci] * wave[rj, ci]
                    + spectrum[part, 2, ri, ci] * wave[ri, cj]
                    + spectrum[part, 3, ri, ci] * wave[rj, cj]
                )
                to = pl.ds((2 * a + part) * half + i * quarter, quarter), pl.ds(b * TILE + j * HALF, HALF)
                y_hi[to], y_lo[to] = split(y)

    def back_rows(a, b):
        cb = pl.ds(b * TILE, TILE)
        sums, diffs = (
            dot32(row_inv[part], triple(y_hi, y_lo, pl.ds((2 * a + part) * half, half), cb, 0)) for part in (0, 1)
        )
        upper = sums[band_width:] + diffs[band_width:]
        lower = sums[: half - band_width] - diffs[: half - band_width]
        put(u, (pl.ds(a * TILE, HALF), cb), upper)
        put(u, (pl.ds(a * TILE + HALF, HALF), cb), lower)

    def tile_left(a, b):
        at = pl.ds(a * TILE, TILE), pl.ds(b * TILE, TILE)
        rest_same = jnp.concatenate([w_rest[at], w_same[at]], 0)
        put(t, at, dot32(left_main[a, b], w_main[at]) + dot32(left_small[a, b], rest_same))

    def update(a, keep, take, factor):
        ra = pl.ds(a * TILE, TILE)
        square = jnp.zeros((8, LANES), jnp.float32)
        parts = []
        for b in range(col_windows):
            at = ra, pl.ds(b * TILE, TILE)
            lhs, lhs_small, rhs, rhs_small = [u_main[at]], [u_rest[at], u_same[at]], [col_main[1, b]], [col_small[1, b]]
            if b % 2 == 0:
                at = ra, pl.ds(b // 2 * TILE, TILE)
                lhs, lhs_small = lhs + [t_main[at]], lhs_small + [t_rest[at], t_same[at]]
                rhs, rhs_small = rhs + [right_main[a, b // 2]], rhs_small + [right_small[a, b // 2]]
            parts.append(
                dot32(jnp.concatenate(lhs, 1), jnp.concatenate(rhs, 0))
                + dot32(jnp.concatenate(lhs_small, 1), jnp.concatenate(rhs_small, 0))
            )
        for j in range(cols // HALF):
            pieces = [parts[b][:, (j - b) * HALF : (j - b + 1) * HALF] for b in range(col_windows) if b <= j <= b + 1]
            cj = pl.ds(j * HALF, HALF)
            residual = keep * state[ra, cj] - times(functools.reduce(jnp.add, pieces), take)
            state[ra, cj] = residual
            total[ra, cj] = total[ra, cj] + relax_step * residual
            put(w, (ra, cj), times(residual, factor))
            square = square + jnp.sum((residual * residual).reshape(TILE // 8, 8, LANES), 0)
        return square

    def step(k, carry):
        sums, last = carry
        keep = jnp.where(k == 0, 0.0, 1.0 - relax_step)
        take = jnp.where(k == 0, 1.0, relax_step) / (BACK_SCALE * scale[...])
        factor = scaled_by(last)
        tiles = [(a, b) for a in range(tile_rows) for b in range(tile_cols)]
        for b in range(col_windows):
            columns(b)
        for b in range(col_windows):
            for a in range(tile_rows):
                spectral(a, b, 0)
                spectral(a, b, 1)
                if tiles:
                    tile_left(*tiles.pop(0))
                if b:
                    back_rows(a, b - 1)
        for at in tiles:
            tile_left(*at)
        for a in range(tile_rows):
            back_rows(a, col_windows - 1)
        square = jnp.zeros((8, LANES), jnp.float32)
        for a in range(tile_rows):
            square = square + update(a, keep, take, factor)
        scale[...] = factor
        sum_square = jnp.sum(square)
        return jnp.where(norm_lane == k, sum_square, sums), sum_square

    sum_square = jnp.sum(square)
    scale[...] = scaled_by(sum_square)
    for i in range(0, rows, TILE):
        for j in range(0, cols, LANES):
            at = pl.ds(i, TILE), pl.ds(j, LANES)
            put(w, at, times(state[at], scale[...]))
    norm_lane = lax.broadcasted_iota(jnp.int32, norms.shape, 1)
    for load in loads[12:]:
        load.wait()
    def two_steps(k, carry):
        return step(2 * k + 1, step(2 * k, carry))

    summed, _ = lax.fori_loop(0, ITERS // 2, two_steps, (jnp.zeros(norms.shape, jnp.float32), sum_square))
    norms[...] = jnp.sqrt(summed / (rows * cols) + tiny_square)
    own_row = pl.multiple_of(here_x * block_rows, block_rows)
    own_col = pl.multiple_of((here_y * 2 + here_c) * block_cols, block_cols)
    out[...] = total[pl.ds(own_row, block_rows), pl.ds(own_col, block_cols)]


def swap(value, axis, bit):
    return lax.ppermute(value, axis, [(i, i ^ bit) for i in range(lax.axis_size(axis))])


def doubled(value, axis, bits):
    for bit in bits:
        value = jnp.concatenate([value, swap(value, axis, bit)], 0)
    return value


def bit_places(bits):
    places = [0]
    for bit in bits:
        places = places + [p | bit for p in places]
    return places


def replicated(source, coeffs, row_factor, col_factor, tile_mask):
    block_rows, block_cols = source.shape
    rows, cols = col_factor.shape[0], row_factor.shape[1]
    band_width = (coeffs.shape[0] - 1) // 2
    hx_size, hy_size = lax.axis_size("hx"), lax.axis_size("hy")
    index_x, index_y = lax.axis_index("hx"), lax.axis_index("hy")
    down = [1 << i for i in reversed(range(hx_size.bit_length() - 1))]
    turned = down[:-2] + down[-2:][::-1]
    y_bits = [1 << i for i in range(1, hy_size.bit_length() - 1)]
    s_part = doubled(source[None], "hy", y_bits)
    r_half = lax.dynamic_slice_in_dim(row_factor, (index_y % 2) * (cols // 2), cols // 2, 1)
    r_near = doubled(r_half.reshape(block_rows, -1, LANES).swapaxes(0, 1)[None], "hx", turned[:-1])
    s_near = doubled(s_part[None], "hx", down[:-2])
    s_near = doubled(s_near, "hx", down[-2:-1])
    s_near, coeffs = lax.optimization_barrier((s_near, coeffs))
    ready = setup(coeffs, cols)
    c_near = doubled(col_factor[None], "hy", y_bits[:-1])
    turns = [swap(s_near, "hx", down[-1]), swap(r_near, "hx", turned[-1]), swap(c_near, "hy", y_bits[-1])]
    s_held, *ready = lax.optimization_barrier((s_near, *ready))
    pieces = []
    for near, held, turn in zip((s_near, r_near, c_near), (s_held, r_near, c_near), turns):
        pieces += [near, turn, swap(held, "hy", 1), swap(turn, "hy", 1)]
    spectrum, col_main, col_small = ready
    row_fwd, row_inv = (jnp.asarray(m) for m in row_mats(band_width))
    place = jnp.stack([index_x, index_y // 2, index_y % 2])
    half, col_windows = HALF + band_width, cols // HALF - 1
    vmem = pl.BlockSpec(memory_space=pltpu.VMEM)
    smem = pl.BlockSpec(memory_space=pltpu.SMEM)
    f32, bf16 = jnp.float32, jnp.bfloat16
    tiles = (rows // TILE, cols // TILE)
    wide = col_windows * TILE
    shapes = [((rows, cols), f32)] * 2 + [((rows + 2 * band_width, wide), f32)]
    shapes += [((2 * half * tiles[0], wide), bf16)] * 2
    for shape in ((rows, cols), (rows, wide), (rows, cols)):
        shapes += [(shape, bf16), (shape, small), (shape, small)]
    shapes += [(tiles + (TILE, TILE), bf16), (tiles + (TILE, 2 * TILE), small)]
    shapes += [(tiles + (TILE, TILE), bf16), (tiles + (2 * TILE, TILE), small), ((8, LANES), f32)]
    operands = (*pieces, spectrum, row_fwd, row_inv, col_main, col_small)
    shapes += [(v.shape, v.dtype) for v in operands]
    result, norms = pl.pallas_call(
        functools.partial(replicated_kernel, (bit_places(down), bit_places(turned))),
        out_shape=(
            jax.ShapeDtypeStruct((block_rows, block_cols), f32),
            jax.ShapeDtypeStruct((1, ITERS), f32),
        ),
        in_specs=[smem, smem] + [pl.BlockSpec(memory_space=pl.ANY)] * 17,
        out_specs=(vmem, vmem),
        scratch_shapes=[pltpu.VMEM(*s) for s in shapes] + [pltpu.SemaphoreType.DMA((len(operands),))],
        compiler_params=pltpu.CompilerParams(vmem_limit_bytes=50 * 1024 * 1024),
        name="replicated_steps",
    )(place, tile_mask, *operands)
    return result, norms[0]


def fits(rows, cols, block_rows, block_cols, band_width, hx_size, hy_size):
    powers = all(n & (n - 1) == 0 for n in (hx_size, hy_size))
    whole = rows % TILE == 0 and cols % TILE == 0 and rows > TILE and cols > TILE
    aligned = TILE % block_rows == 0 and block_rows % 16 == 0 and block_cols == LANES and cols % (2 * LANES) == 0
    small = rows * cols * 4 <= GRID_BYTES and 4 * band_width <= TILE and band_width % 32 == 0
    return powers and whole and aligned and small and hx_size >= 4 and hy_size >= 4


def local(source, coeffs, row_factor, col_factor, tile_mask):
    rows, cols = col_factor.shape[0], row_factor.shape[1]
    band_width = (coeffs.shape[0] - 1) // 2
    sizes = lax.axis_size("hx"), lax.axis_size("hy")
    if fits(rows, cols, *source.shape, band_width, *sizes):
        return replicated(source, coeffs, row_factor, col_factor, tile_mask)
    return distributed(source, coeffs, row_factor, col_factor, tile_mask)


def solution(mesh):
    in_specs = (P("hx", "hy"), P(), P("hx", None), P(None, "hy"), P())
    out_specs = (P("hx", "hy"), P())
    return jax.shard_map(local, mesh=mesh, in_specs=in_specs, out_specs=out_specs, check_vma=False)
```

```python
import functools
import jax
import jax.numpy as jnp
import numpy as np
from jax import lax
from jax.experimental import pallas as pl
from jax.experimental.pallas import tpu as pltpu
from jax.sharding import PartitionSpec as P

TILE = 256
ITERS = 8
HALF = TILE // 2
LANES = 128
GRID_BYTES = 2 * 1024 * 1024
LEFT_SCALE, RIGHT_SCALE, VECTOR_SCALE = 16.0, 8.0, 256.0
BACK_SCALE = LEFT_SCALE * RIGHT_SCALE
small = jnp.float8_e5m2


relax_step = 0.25
highest = lax.Precision.HIGHEST
tiny_square = 1e-06


def with_halo(value, sides, width):
    for axis, dim in sides:
        count, length = (lax.axis_size(axis), value.shape[dim])
        up = [(i, (i + 1) % count) for i in range(count - 1)]
        down = [(j, i) for i, j in up]
        last = lax.slice_in_dim(value, length - width, length, axis=dim)
        initial = lax.slice_in_dim(value, 0, width, axis=dim)
        before = lax.ppermute(last, axis, up)
        after = lax.ppermute(initial, axis, down)
        value = jnp.concatenate([before, value, after], axis=dim)
    return value


def swapped(value, axis, apart):
    return lax.ppermute(value, axis, [(i, i ^ 1 << apart) for i in range(lax.axis_size(axis))])


def row_panels(coeffs, row_count, band_width):
    tap_count = 2 * band_width + 1
    padded_rows = row_count + 2 * band_width
    shape_three = (tap_count, row_count, padded_rows)
    tap_index = lax.broadcasted_iota(jnp.int32, shape_three, 0)
    target = lax.broadcasted_iota(jnp.int32, shape_three, 1)
    source_row = lax.broadcasted_iota(jnp.int32, shape_three, 2)
    picker = (source_row == target + 2 * band_width - tap_index).astype(jnp.float32)
    panels = jnp.einsum("pq,pmi->mqi", coeffs, picker, precision=highest)
    return panels.reshape(row_count, tap_count * padded_rows)


def banded_product(field_now, panels, band_width):
    col_count = field_now.shape[1]
    padded = with_halo(field_now, (("hx", 0), ("hy", 1)), band_width)
    pieces = [
        padded[:, 2 * band_width - offset : 2 * band_width - offset + col_count]
        for offset in range(2 * band_width + 1)
    ]
    stacked = jnp.concatenate(pieces, axis=0)
    return jnp.dot(panels, stacked, precision=highest, preferred_element_type=jnp.float32)


def joined(block, partner, upper_half, axis_dim):
    return jnp.where(
        upper_half,
        jnp.concatenate([partner, block], axis_dim),
        jnp.concatenate([block, partner], axis_dim),
    )


def distributed(source, coeffs, row_factor, col_factor, tile_mask):
    row_count, col_count = source.shape
    band_width = (coeffs.shape[0] - 1) // 2
    row_group = TILE // row_count
    col_group = TILE // col_count
    row_index = lax.axis_index("hx")
    col_index = lax.axis_index("hy")
    tile_row = row_index // row_group
    tile_col = col_index // col_group
    panels = row_panels(coeffs, row_count, band_width)
    row_factor_tile = lax.dynamic_slice_in_dim(row_factor, tile_col * TILE, TILE, 1)
    col_factor_tile = lax.dynamic_slice_in_dim(col_factor, tile_row * TILE, TILE, 0)
    mask_rows = lax.broadcasted_iota(jnp.int32, tile_mask.shape, 0)
    mask_cols = lax.broadcasted_iota(jnp.int32, tile_mask.shape, 1)
    chosen = (mask_rows == tile_row) & (mask_cols == tile_col)
    active = jnp.sum(jnp.where(chosen, tile_mask, 0)).astype(jnp.float32)
    solution = source
    squares = []
    for step_index in range(ITERS):
        wide_block = solution
        bit_level = 0
        partner = swapped(wide_block, "hy", bit_level)
        upper_half = col_index // (1 << bit_level) % 2 == 1
        wide_block = joined(wide_block, partner, upper_half, 1)
        mixed_cols = jnp.dot(
            wide_block, col_factor_tile, precision=highest, preferred_element_type=jnp.float32
        )
        tall_block = mixed_cols
        for bit_level in range(row_group.bit_length() - 1):
            partner = swapped(tall_block, "hx", bit_level)
            upper_half = row_index // (1 << bit_level) % 2 == 1
            tall_block = joined(tall_block, partner, upper_half, 0)
        result = jnp.dot(
            row_factor_tile, tall_block, precision=highest, preferred_element_type=jnp.float32
        )
        applied = solution + banded_product(solution, panels, band_width) + active * result
        residual = source - applied
        local_square = jnp.sum(residual * residual)
        squares.append(lax.psum(local_square, ("hx", "hy")))
        solution = solution + relax_step * residual
    summed = jnp.stack(squares)
    cell_count = row_count * col_count * lax.axis_size("hx") * lax.axis_size("hy")
    norm_values = jnp.sqrt(summed / cell_count + tiny_square)
    return (solution, norm_values)


def split_np(value):
    high = value.astype(jnp.bfloat16)
    return high, (value - high.astype(np.float64)).astype(jnp.bfloat16)


def packed_freqs(length):
    half = length // 2
    freq = np.concatenate([np.arange(half), np.arange(half)])
    freq[half] = half
    return freq


def cyclic_mats(length):
    half = length // 2
    phase = 2 * np.pi * ((packed_freqs(length)[:, None] * np.arange(length)[None, :]) % length) / length
    forward = np.concatenate([np.cos(phase[: half + 1]), np.sin(phase[half + 1 :])], 0)
    weight = np.full((length, 1), 2.0 / length)
    weight[0] = weight[half] = 1.0 / length
    return forward, (forward * weight).T


def negacyclic_mats(length):
    half = length // 2
    odd = 2 * np.arange(half) + 1
    phase = 2 * np.pi * ((odd[:, None] * np.arange(length)[None, :]) % (2 * length)) / (2 * length)
    forward = np.concatenate([np.cos(phase), np.sin(phase)], 0)
    return forward, (forward * (2.0 / length)).T


def row_mats(band_width):
    half = (TILE + 2 * band_width) // 2
    fwd, inv = [], []
    for forward, inverse in (cyclic_mats(half), negacyclic_mats(half)):
        fh, fl = split_np(forward)
        gh, gl = split_np(inverse * 0.5)
        fwd.append(np.concatenate([fh, fh, fl], 1))
        inv.append(np.concatenate([gh, gh, gl], 1))
    return np.stack(fwd), np.stack(inv)


def col_mats():
    forward, inverse = cyclic_mats(TILE)
    return np.stack(split_np(forward.T) + split_np(inverse.T * BACK_SCALE))


def tap_waves(band_width):
    offset = np.arange(-band_width, band_width + 1)
    half = (TILE + 2 * band_width) // 2
    odd = 2 * np.arange(half // 2) + 1
    row_freq = np.concatenate([2 * packed_freqs(half), odd, odd])
    row_phase = 2 * np.pi * ((row_freq[:, None] * offset[None, :]) % (2 * half)) / (2 * half)
    col_phase = 2 * np.pi * ((packed_freqs(TILE)[:, None] * offset[None, :]) % TILE) / TILE
    rows = np.stack([np.cos(row_phase), np.sin(row_phase)]).astype(np.float32)
    cols = np.stack([np.cos(col_phase).T, np.sin(col_phase).T]).astype(np.float32)
    return rows, cols


def setup_kernel(coeffs, row_waves, col_waves, col_base, spectrum, col_main, col_small):
    half = spectrum.shape[2]
    band_width = (coeffs.shape[0] - 1) // 2
    for j in (0, 1):
        cols = jnp.dot(coeffs[...], col_waves[j], precision=highest, preferred_element_type=jnp.float32)
        lane = lax.broadcasted_iota(jnp.int32, (1, TILE), 1)
        if j:
            cols = jnp.where(lane < HALF, -cols, cols)
        for i in (0, 1):
            mixed = jnp.dot(row_waves[i], cols, precision=highest, preferred_element_type=jnp.float32)
            if i:
                place = lax.broadcasted_iota(jnp.int32, (2 * half, 1), 0) % half
                mixed = jnp.where(place < half // 2, -mixed, mixed)
            for part in (0, 1):
                spectrum[part, 2 * j + i] = mixed[part * half : (part + 1) * half]
    count = col_main.shape[1]
    for w in range(count):
        for way in (0, 1):
            for part in (0, 1):
                cells = col_base[2 * way + part].astype(jnp.float32)
                place = lax.broadcasted_iota(jnp.int32, cells.shape, way)
                margin = HALF // 2 if way else band_width
                if (w > 0) if way else (w == count - 1):
                    cells = jnp.where(place >= margin, cells, 0.0)
                if (w < count - 1) if way else (w == 0):
                    cells = jnp.where(place < TILE - margin, cells, 0.0)
                if part == 0:
                    col_main[way, w] = cells.astype(jnp.bfloat16)
                col_small[way, w, part * TILE : (part + 1) * TILE] = cells.astype(small)


def setup(coeffs, cols):
    band_width = (coeffs.shape[0] - 1) // 2
    windows = cols // HALF - 1
    waves = [jnp.asarray(v) for v in tap_waves(band_width)]
    vmem = pl.BlockSpec(memory_space=pltpu.VMEM)
    return pl.pallas_call(
        setup_kernel,
        out_shape=(
            jax.ShapeDtypeStruct((2, 4, HALF + band_width, TILE), jnp.float32),
            jax.ShapeDtypeStruct((2, windows, TILE, TILE), jnp.bfloat16),
            jax.ShapeDtypeStruct((2, windows, 2 * TILE, TILE), small),
        ),
        in_specs=[vmem] * 4,
        out_specs=(vmem,) * 3,
        compiler_params=pltpu.CompilerParams(vmem_limit_bytes=16 * 1024 * 1024),
        name="setup",
    )(coeffs, *waves, jnp.asarray(col_mats()))


def split(value):
    high = value.astype(jnp.bfloat16)
    return high, (value - high.astype(jnp.float32)).astype(jnp.bfloat16)


def split_small(value):
    high = value.astype(jnp.bfloat16)
    low = (value - high.astype(jnp.float32)).astype(jnp.bfloat16)
    most = jnp.asarray(jnp.finfo(small).max, jnp.bfloat16)
    return high, jnp.clip(low, -most, most).astype(small), jnp.clip(high, -most, most).astype(small)


def dot32(left, right):
    return jnp.dot(left, right, preferred_element_type=jnp.float32)


def replicated_kernel(hx_bits, place, mask, *refs):
    sources, (out, norms), held = refs[:17], refs[17:19], refs[38:55]
    loads = [pltpu.make_async_copy(a, b, refs[55].at[i]) for i, (a, b) in enumerate(zip(sources, held))]
    for load in loads:
        load.start()
    s_near, s_turn, s_far, s_both, r_near, r_turn, r_far, r_both, c_near, c_turn, c_far, c_both = held[:12]
    spectrum, row_fwd, row_inv, col_main, col_small = held[12:]
    state, total, z, y_hi, y_lo, w_main, w_rest, w_same, u_main, u_rest, u_same, t_main, t_rest, t_same = refs[19:33]
    left_main, left_small, right_main, right_small, scale = refs[33:38]
    w, u, t = (w_main, w_rest, w_same), (u_main, u_rest, u_same), (t_main, t_rest, t_same)
    rows, cols = state.shape
    col_windows = col_main.shape[1]
    half = row_fwd.shape[1]
    quarter = half // 2
    band_width = half - HALF
    tile_rows, tile_cols = rows // TILE, cols // TILE
    block_rows, block_cols = s_near.shape[-2:]
    near_count = s_near.shape[0]
    here_x, here_y, here_c = place[0], place[1], place[2]
    square = jnp.zeros((8, LANES), jnp.float32)
    for load in loads[:4]:
        load.wait()
    for pos in range(2 * near_count):
        s_row = (here_x ^ hx_bits[0][pos]) * block_rows
        s_row = pl.multiple_of(s_row, block_rows)
        for far, ref in enumerate((s_near, s_far) if pos < near_count else (s_turn, s_both)):
            for k in range(ref.shape[1]):
                s_col = ((here_y ^ k) * 2 + (here_c ^ far)) * block_cols
                s_col = pl.multiple_of(s_col, block_cols)
                value = ref[pos % near_count, k]
                state[pl.ds(s_row, block_rows), pl.ds(s_col, block_cols)] = value
                total[pl.ds(s_row, block_rows), pl.ds(s_col, block_cols)] = value
                square = square + jnp.sum((value * value).reshape(block_rows // 8, 8, block_cols), 0)
    for load in loads[4:8]:
        load.wait()
    share = TILE // block_rows
    for pos in range(2 * near_count):
        index = here_x ^ hx_bits[1][pos]
        a = index // share
        sub = pl.multiple_of((index % share) * block_rows, block_rows)
        for far, ref in enumerate((r_near, r_far) if pos < near_count else (r_turn, r_both)):
            side = here_c ^ far
            for k in range(ref.shape[1]):
                lane = side * (cols // 2) + k * LANES
                b = lane // TILE
                at = pl.multiple_of(lane % TILE, LANES)
                cells = ref[pos % near_count, k] * (LEFT_SCALE * mask[a, b].astype(jnp.float32))
                high, rest, same = split_small(cells)
                left_main[a, b, pl.ds(sub, block_rows), pl.ds(at, LANES)] = high
                left_small[a, b, pl.ds(sub, block_rows), pl.ds(at, LANES)] = same
                left_small[a, b, pl.ds(sub, block_rows), pl.ds(pl.multiple_of(at + TILE, LANES), LANES)] = rest
    for load in loads[8:12]:
        load.wait()
    for k in range(2 * c_near.shape[0]):
        for far, ref in enumerate((c_near, c_far) if k < c_near.shape[0] else (c_turn, c_both)):
            lane = ((here_y ^ k) * 2 + (here_c ^ far)) * block_cols
            b = lane // TILE
            at = pl.multiple_of(lane % TILE, block_cols)
            for a in range(tile_rows):
                high, rest, same = split_small(ref[k % c_near.shape[0], pl.ds(a * TILE, TILE), :] * RIGHT_SCALE)
                right_main[a, b, :, pl.ds(at, block_cols)] = high
                right_small[a, b, pl.ds(0, TILE), pl.ds(at, block_cols)] = same
                right_small[a, b, pl.ds(TILE, TILE), pl.ds(at, block_cols)] = rest

    for edge in (0, rows + band_width):
        z[pl.ds(edge, band_width), :] = jnp.zeros((band_width, z.shape[1]), jnp.float32)

    def triple(hi_ref, lo_ref, row_at, col_at, axis):
        high = hi_ref[row_at, col_at]
        return jnp.concatenate([high, lo_ref[row_at, col_at], high], axis)

    def put(refs, at, value):
        for ref, part in zip(refs, split_small(value)):
            ref[at] = part

    def scaled_by(sum_square):
        return VECTOR_SCALE * lax.rsqrt(jnp.maximum(jnp.full((8, LANES), sum_square), 1e-30))

    def times(cells, factor):
        return (cells.reshape(-1, 8, LANES) * factor).reshape(cells.shape)

    def columns(b):
        at = slice(None), pl.ds(b * HALF, TILE)
        rest_same = jnp.concatenate([w_rest[at], w_same[at]], 1)
        z[pl.ds(band_width, rows), pl.ds(b * TILE, TILE)] = dot32(w_main[at], col_main[0, b]) + dot32(
            rest_same, col_small[0, b]
        )

    def spectral(a, b, part):
        cb = pl.ds(b * TILE, TILE)
        upper = z[pl.ds(a * TILE, half), cb]
        lower = z[pl.ds(a * TILE + half, half), cb]
        high, low = split(upper - lower if part else upper + lower)
        wave = dot32(row_fwd[part], jnp.concatenate([high, low, high], 0))
        for i in (0, 1):
            for j in (0, 1):
                ri, rj = slice(i * quarter, (i + 1) * quarter), slice((1 - i) * quarter, (2 - i) * quarter)
                ci, cj = slice(j * HALF, (j + 1) * HALF), slice((1 - j) * HALF, (2 - j) * HALF)
                y = (
                    spectrum[part, 0, ri, ci] * wave[ri, ci]
                    + spectrum[part, 1, ri, ci] * wave[rj, ci]
                    + spectrum[part, 2, ri, ci] * wave[ri, cj]
                    + spectrum[part, 3, ri, ci] * wave[rj, cj]
                )
                to = pl.ds((2 * a + part) * half + i * quarter, quarter), pl.ds(b * TILE + j * HALF, HALF)
                y_hi[to], y_lo[to] = split(y)

    def back_rows(a, b):
        cb = pl.ds(b * TILE, TILE)
        sums, diffs = (
            dot32(row_inv[part], triple(y_hi, y_lo, pl.ds((2 * a + part) * half, half), cb, 0)) for part in (0, 1)
        )
        upper = sums[band_width:] + diffs[band_width:]
        lower = sums[: half - band_width] - diffs[: half - band_width]
        put(u, (pl.ds(a * TILE, HALF), cb), upper)
        put(u, (pl.ds(a * TILE + HALF, HALF), cb), lower)

    def tile_left(a, b):
        at = pl.ds(a * TILE, TILE), pl.ds(b * TILE, TILE)
        rest_same = jnp.concatenate([w_rest[at], w_same[at]], 0)
        put(t, at, dot32(left_main[a, b], w_main[at]) + dot32(left_small[a, b], rest_same))

    def update(a, keep, take, factor):
        ra = pl.ds(a * TILE, TILE)
        square = jnp.zeros((8, LANES), jnp.float32)
        before = None
        for b in range(col_windows + 1):
            done = before
            if b < col_windows:
                at = ra, pl.ds(b * TILE, TILE)
                lhs, lhs_small, rhs, rhs_small = [u_main[at]], [u_rest[at], u_same[at]], [col_main[1, b]], [col_small[1, b]]
                if b % 2 == 0:
                    at = ra, pl.ds(b // 2 * TILE, TILE)
                    lhs, lhs_small = lhs + [t_main[at]], lhs_small + [t_rest[at], t_same[at]]
                    rhs, rhs_small = rhs + [right_main[a, b // 2]], rhs_small + [right_small[a, b // 2]]
                cells = dot32(jnp.concatenate(lhs, 1), jnp.concatenate(rhs, 0)) + dot32(
                    jnp.concatenate(lhs_small, 1), jnp.concatenate(rhs_small, 0)
                )
                done = cells[:, :HALF] if before is None else before + cells[:, :HALF]
                before = cells[:, HALF:]
            cj = pl.ds(b * HALF, HALF)
            residual = keep * state[ra, cj] - times(done, take)
            state[ra, cj] = residual
            total[ra, cj] = total[ra, cj] + relax_step * residual
            put(w, (ra, cj), times(residual, factor))
            square = square + jnp.sum((residual * residual).reshape(TILE // 8, 8, LANES), 0)
        return square

    def step(k, carry):
        sums, last = carry
        keep = jnp.where(k == 0, 0.0, 1.0 - relax_step)
        take = jnp.where(k == 0, 1.0, relax_step) / (BACK_SCALE * scale[...])
        factor = scaled_by(last)
        tiles = [(a, b) for a in range(tile_rows) for b in range(tile_cols)]
        for b in range(col_windows):
            columns(b)
        for b in range(col_windows):
            for a in range(tile_rows):
                spectral(a, b, 0)
                spectral(a, b, 1)
                if tiles:
                    tile_left(*tiles.pop(0))
                if b:
                    back_rows(a, b - 1)
        for at in tiles:
            tile_left(*at)
        for a in range(tile_rows):
            back_rows(a, col_windows - 1)
        square = jnp.zeros((8, LANES), jnp.float32)
        for a in range(tile_rows):
            square = square + update(a, keep, take, factor)
        scale[...] = factor
        sum_square = jnp.sum(square)
        return jnp.where(norm_lane == k, sum_square, sums), sum_square

    sum_square = jnp.sum(square)
    scale[...] = scaled_by(sum_square)
    for i in range(0, rows, TILE):
        for j in range(0, cols, LANES):
            at = pl.ds(i, TILE), pl.ds(j, LANES)
            put(w, at, times(state[at], scale[...]))
    norm_lane = lax.broadcasted_iota(jnp.int32, norms.shape, 1)
    for load in loads[12:]:
        load.wait()
    def two_steps(k, carry):
        return step(2 * k + 1, step(2 * k, carry))

    summed, _ = lax.fori_loop(0, ITERS // 2, two_steps, (jnp.zeros(norms.shape, jnp.float32), sum_square))
    norms[...] = jnp.sqrt(summed / (rows * cols) + tiny_square)
    own_row = pl.multiple_of(here_x * block_rows, block_rows)
    own_col = pl.multiple_of((here_y * 2 + here_c) * block_cols, block_cols)
    out[...] = total[pl.ds(own_row, block_rows), pl.ds(own_col, block_cols)]


def swap(value, axis, bit):
    return lax.ppermute(value, axis, [(i, i ^ bit) for i in range(lax.axis_size(axis))])


def doubled(value, axis, bits):
    for bit in bits:
        value = jnp.concatenate([value, swap(value, axis, bit)], 0)
    return value


def bit_places(bits):
    places = [0]
    for bit in bits:
        places = places + [p | bit for p in places]
    return places


def replicated(source, coeffs, row_factor, col_factor, tile_mask):
    block_rows, block_cols = source.shape
    rows, cols = col_factor.shape[0], row_factor.shape[1]
    band_width = (coeffs.shape[0] - 1) // 2
    hx_size, hy_size = lax.axis_size("hx"), lax.axis_size("hy")
    index_x, index_y = lax.axis_index("hx"), lax.axis_index("hy")
    down = [1 << i for i in reversed(range(hx_size.bit_length() - 1))]
    turned = down[:-2] + down[-2:][::-1]
    y_bits = [1 << i for i in range(1, hy_size.bit_length() - 1)]
    s_part = doubled(source[None], "hy", y_bits)
    r_half = lax.dynamic_slice_in_dim(row_factor, (index_y % 2) * (cols // 2), cols // 2, 1)
    r_near = doubled(r_half.reshape(block_rows, -1, LANES).swapaxes(0, 1)[None], "hx", turned[:-1])
    s_near = doubled(s_part[None], "hx", down[:-2])
    s_near = doubled(s_near, "hx", down[-2:-1])
    s_near, coeffs = lax.optimization_barrier((s_near, coeffs))
    ready = setup(coeffs, cols)
    c_near = doubled(col_factor[None], "hy", y_bits[:-1])
    turns = [swap(s_near, "hx", down[-1]), swap(r_near, "hx", turned[-1]), swap(c_near, "hy", y_bits[-1])]
    s_held, *ready = lax.optimization_barrier((s_near, *ready))
    pieces = []
    for near, held, turn in zip((s_near, r_near, c_near), (s_held, r_near, c_near), turns):
        pieces += [near, turn, swap(held, "hy", 1), swap(turn, "hy", 1)]
    spectrum, col_main, col_small = ready
    row_fwd, row_inv = (jnp.asarray(m) for m in row_mats(band_width))
    place = jnp.stack([index_x, index_y // 2, index_y % 2])
    half, col_windows = HALF + band_width, cols // HALF - 1
    vmem = pl.BlockSpec(memory_space=pltpu.VMEM)
    smem = pl.BlockSpec(memory_space=pltpu.SMEM)
    f32, bf16 = jnp.float32, jnp.bfloat16
    tiles = (rows // TILE, cols // TILE)
    wide = col_windows * TILE
    shapes = [((rows, cols), f32)] * 2 + [((rows + 2 * band_width, wide), f32)]
    shapes += [((2 * half * tiles[0], wide), bf16)] * 2
    for shape in ((rows, cols), (rows, wide), (rows, cols)):
        shapes += [(shape, bf16), (shape, small), (shape, small)]
    shapes += [(tiles + (TILE, TILE), bf16), (tiles + (TILE, 2 * TILE), small)]
    shapes += [(tiles + (TILE, TILE), bf16), (tiles + (2 * TILE, TILE), small), ((8, LANES), f32)]
    operands = (*pieces, spectrum, row_fwd, row_inv, col_main, col_small)
    shapes += [(v.shape, v.dtype) for v in operands]
    result, norms = pl.pallas_call(
        functools.partial(replicated_kernel, (bit_places(down), bit_places(turned))),
        out_shape=(
            jax.ShapeDtypeStruct((block_rows, block_cols), f32),
            jax.ShapeDtypeStruct((1, ITERS), f32),
        ),
        in_specs=[smem, smem] + [pl.BlockSpec(memory_space=pl.ANY)] * 17,
        out_specs=(vmem, vmem),
        scratch_shapes=[pltpu.VMEM(*s) for s in shapes] + [pltpu.SemaphoreType.DMA((len(operands),))],
        compiler_params=pltpu.CompilerParams(vmem_limit_bytes=50432 * 1024),
        name="replicated_steps",
    )(place, tile_mask, *operands)
    return result, norms[0]


def fits(rows, cols, block_rows, block_cols, band_width, hx_size, hy_size):
    powers = all(n & (n - 1) == 0 for n in (hx_size, hy_size))
    whole = rows % TILE == 0 and cols % TILE == 0 and rows > TILE and cols > TILE
    aligned = TILE % block_rows == 0 and block_rows % 16 == 0 and block_cols == LANES and cols % (2 * LANES) == 0
    small = rows * cols * 4 <= GRID_BYTES and 4 * band_width <= TILE and band_width % 32 == 0
    return powers and whole and aligned and small and hx_size >= 4 and hy_size >= 4


def local(source, coeffs, row_factor, col_factor, tile_mask):
    rows, cols = col_factor.shape[0], row_factor.shape[1]
    band_width = (coeffs.shape[0] - 1) // 2
    sizes = lax.axis_size("hx"), lax.axis_size("hy")
    if fits(rows, cols, *source.shape, band_width, *sizes):
        return replicated(source, coeffs, row_factor, col_factor, tile_mask)
    return distributed(source, coeffs, row_factor, col_factor, tile_mask)


def solution(mesh):
    in_specs = (P("hx", "hy"), P(), P("hx", None), P(None, "hy"), P())
    out_specs = (P("hx", "hy"), P())
    return jax.shard_map(local, mesh=mesh, in_specs=in_specs, out_specs=out_specs, check_vma=False)
```

```python
import functools
import jax
import jax.numpy as jnp
import numpy as np
from jax import lax
from jax.experimental import pallas as pl
from jax.experimental.pallas import tpu as pltpu
from jax.sharding import PartitionSpec as P

TILE = 256
ITERS = 8
HALF = TILE // 2
LANES = 128
GRID_BYTES = 2 * 1024 * 1024
LEFT_SCALE, RIGHT_SCALE, VECTOR_SCALE = 16.0, 8.0, 256.0
BACK_SCALE = LEFT_SCALE * RIGHT_SCALE
small = jnp.float8_e5m2


relax_step = 0.25
highest = lax.Precision.HIGHEST
tiny_square = 1e-06


def with_halo(value, sides, width):
    for axis, dim in sides:
        count, length = (lax.axis_size(axis), value.shape[dim])
        up = [(i, (i + 1) % count) for i in range(count - 1)]
        down = [(j, i) for i, j in up]
        last = lax.slice_in_dim(value, length - width, length, axis=dim)
        initial = lax.slice_in_dim(value, 0, width, axis=dim)
        before = lax.ppermute(last, axis, up)
        after = lax.ppermute(initial, axis, down)
        value = jnp.concatenate([before, value, after], axis=dim)
    return value


def swapped(value, axis, apart):
    return lax.ppermute(value, axis, [(i, i ^ 1 << apart) for i in range(lax.axis_size(axis))])


def row_panels(coeffs, row_count, band_width):
    tap_count = 2 * band_width + 1
    padded_rows = row_count + 2 * band_width
    shape_three = (tap_count, row_count, padded_rows)
    tap_index = lax.broadcasted_iota(jnp.int32, shape_three, 0)
    target = lax.broadcasted_iota(jnp.int32, shape_three, 1)
    source_row = lax.broadcasted_iota(jnp.int32, shape_three, 2)
    picker = (source_row == target + 2 * band_width - tap_index).astype(jnp.float32)
    panels = jnp.einsum("pq,pmi->mqi", coeffs, picker, precision=highest)
    return panels.reshape(row_count, tap_count * padded_rows)


def banded_product(field_now, panels, band_width):
    col_count = field_now.shape[1]
    padded = with_halo(field_now, (("hx", 0), ("hy", 1)), band_width)
    pieces = [
        padded[:, 2 * band_width - offset : 2 * band_width - offset + col_count]
        for offset in range(2 * band_width + 1)
    ]
    stacked = jnp.concatenate(pieces, axis=0)
    return jnp.dot(panels, stacked, precision=highest, preferred_element_type=jnp.float32)


def joined(block, partner, upper_half, axis_dim):
    return jnp.where(
        upper_half,
        jnp.concatenate([partner, block], axis_dim),
        jnp.concatenate([block, partner], axis_dim),
    )


def distributed(source, coeffs, row_factor, col_factor, tile_mask):
    row_count, col_count = source.shape
    band_width = (coeffs.shape[0] - 1) // 2
    row_group = TILE // row_count
    col_group = TILE // col_count
    row_index = lax.axis_index("hx")
    col_index = lax.axis_index("hy")
    tile_row = row_index // row_group
    tile_col = col_index // col_group
    panels = row_panels(coeffs, row_count, band_width)
    row_factor_tile = lax.dynamic_slice_in_dim(row_factor, tile_col * TILE, TILE, 1)
    col_factor_tile = lax.dynamic_slice_in_dim(col_factor, tile_row * TILE, TILE, 0)
    mask_rows = lax.broadcasted_iota(jnp.int32, tile_mask.shape, 0)
    mask_cols = lax.broadcasted_iota(jnp.int32, tile_mask.shape, 1)
    chosen = (mask_rows == tile_row) & (mask_cols == tile_col)
    active = jnp.sum(jnp.where(chosen, tile_mask, 0)).astype(jnp.float32)
    solution = source
    squares = []
    for step_index in range(ITERS):
        wide_block = solution
        bit_level = 0
        partner = swapped(wide_block, "hy", bit_level)
        upper_half = col_index // (1 << bit_level) % 2 == 1
        wide_block = joined(wide_block, partner, upper_half, 1)
        mixed_cols = jnp.dot(
            wide_block, col_factor_tile, precision=highest, preferred_element_type=jnp.float32
        )
        tall_block = mixed_cols
        for bit_level in range(row_group.bit_length() - 1):
            partner = swapped(tall_block, "hx", bit_level)
            upper_half = row_index // (1 << bit_level) % 2 == 1
            tall_block = joined(tall_block, partner, upper_half, 0)
        result = jnp.dot(
            row_factor_tile, tall_block, precision=highest, preferred_element_type=jnp.float32
        )
        applied = solution + banded_product(solution, panels, band_width) + active * result
        residual = source - applied
        local_square = jnp.sum(residual * residual)
        squares.append(lax.psum(local_square, ("hx", "hy")))
        solution = solution + relax_step * residual
    summed = jnp.stack(squares)
    cell_count = row_count * col_count * lax.axis_size("hx") * lax.axis_size("hy")
    norm_values = jnp.sqrt(summed / cell_count + tiny_square)
    return (solution, norm_values)


def split_np(value):
    high = value.astype(jnp.bfloat16)
    return high, (value - high.astype(np.float64)).astype(jnp.bfloat16)


def packed_freqs(length):
    half = length // 2
    freq = np.concatenate([np.arange(half), np.arange(half)])
    freq[half] = half
    return freq


def cyclic_mats(length):
    half = length // 2
    phase = 2 * np.pi * ((packed_freqs(length)[:, None] * np.arange(length)[None, :]) % length) / length
    forward = np.concatenate([np.cos(phase[: half + 1]), np.sin(phase[half + 1 :])], 0)
    weight = np.full((length, 1), 2.0 / length)
    weight[0] = weight[half] = 1.0 / length
    return forward, (forward * weight).T


def negacyclic_mats(length):
    half = length // 2
    odd = 2 * np.arange(half) + 1
    phase = 2 * np.pi * ((odd[:, None] * np.arange(length)[None, :]) % (2 * length)) / (2 * length)
    forward = np.concatenate([np.cos(phase), np.sin(phase)], 0)
    return forward, (forward * (2.0 / length)).T


def row_mats(band_width):
    half = (TILE + 2 * band_width) // 2
    fwd, inv = [], []
    for forward, inverse in (cyclic_mats(half), negacyclic_mats(half)):
        fh, fl = split_np(forward)
        gh, gl = split_np(inverse * 0.5)
        fwd.append(np.concatenate([fh, fh, fl], 1))
        inv.append(np.concatenate([gh, gh, gl], 1))
    return np.stack(fwd), np.stack(inv)


def col_mats():
    forward, inverse = cyclic_mats(TILE)
    return np.stack(split_np(forward.T) + split_np(inverse.T * BACK_SCALE))


def tap_waves(band_width):
    offset = np.arange(-band_width, band_width + 1)
    half = (TILE + 2 * band_width) // 2
    odd = 2 * np.arange(half // 2) + 1
    row_freq = np.concatenate([2 * packed_freqs(half), odd, odd])
    row_phase = 2 * np.pi * ((row_freq[:, None] * offset[None, :]) % (2 * half)) / (2 * half)
    col_phase = 2 * np.pi * ((packed_freqs(TILE)[:, None] * offset[None, :]) % TILE) / TILE
    rows = np.stack([np.cos(row_phase), np.sin(row_phase)]).astype(np.float32)
    cols = np.stack([np.cos(col_phase).T, np.sin(col_phase).T]).astype(np.float32)
    return rows, cols


def setup_kernel(coeffs, row_waves, col_waves, col_base, spectrum, col_main, col_small):
    half = spectrum.shape[2]
    band_width = (coeffs.shape[0] - 1) // 2
    for j in (0, 1):
        cols = jnp.dot(coeffs[...], col_waves[j], precision=highest, preferred_element_type=jnp.float32)
        lane = lax.broadcasted_iota(jnp.int32, (1, TILE), 1)
        if j:
            cols = jnp.where(lane < HALF, -cols, cols)
        for i in (0, 1):
            mixed = jnp.dot(row_waves[i], cols, precision=highest, preferred_element_type=jnp.float32)
            if i:
                place = lax.broadcasted_iota(jnp.int32, (2 * half, 1), 0) % half
                mixed = jnp.where(place < half // 2, -mixed, mixed)
            for part in (0, 1):
                spectrum[part, 2 * j + i] = mixed[part * half : (part + 1) * half]
    count = col_main.shape[1]
    for w in range(count):
        for way in (0, 1):
            for part in (0, 1):
                cells = col_base[2 * way + part].astype(jnp.float32)
                place = lax.broadcasted_iota(jnp.int32, cells.shape, way)
                margin = HALF // 2 if way else band_width
                if (w > 0) if way else (w == count - 1):
                    cells = jnp.where(place >= margin, cells, 0.0)
                if (w < count - 1) if way else (w == 0):
                    cells = jnp.where(place < TILE - margin, cells, 0.0)
                if part == 0:
                    col_main[way, w] = cells.astype(jnp.bfloat16)
                col_small[way, w, part * TILE : (part + 1) * TILE] = cells.astype(small)


def setup(coeffs, cols):
    band_width = (coeffs.shape[0] - 1) // 2
    windows = cols // HALF - 1
    waves = [jnp.asarray(v) for v in tap_waves(band_width)]
    vmem = pl.BlockSpec(memory_space=pltpu.VMEM)
    return pl.pallas_call(
        setup_kernel,
        out_shape=(
            jax.ShapeDtypeStruct((2, 4, HALF + band_width, TILE), jnp.float32),
            jax.ShapeDtypeStruct((2, windows, TILE, TILE), jnp.bfloat16),
            jax.ShapeDtypeStruct((2, windows, 2 * TILE, TILE), small),
        ),
        in_specs=[vmem] * 4,
        out_specs=(vmem,) * 3,
        compiler_params=pltpu.CompilerParams(vmem_limit_bytes=16 * 1024 * 1024),
        name="setup",
    )(coeffs, *waves, jnp.asarray(col_mats()))


def split(value):
    high = value.astype(jnp.bfloat16)
    return high, (value - high.astype(jnp.float32)).astype(jnp.bfloat16)


def split_small(value):
    high = value.astype(jnp.bfloat16)
    low = (value - high.astype(jnp.float32)).astype(jnp.bfloat16)
    most = jnp.asarray(jnp.finfo(small).max, jnp.bfloat16)
    return high, jnp.clip(low, -most, most).astype(small), jnp.clip(high, -most, most).astype(small)


def dot32(left, right):
    return jnp.dot(left, right, preferred_element_type=jnp.float32)


def replicated_kernel(hx_bits, place, mask, *refs):
    sources, (out, norms), held = refs[:17], refs[17:19], refs[38:55]
    loads = [pltpu.make_async_copy(a, b, refs[55].at[i]) for i, (a, b) in enumerate(zip(sources, held))]
    for load in loads:
        load.start()
    s_near, s_turn, s_far, s_both, r_near, r_turn, r_far, r_both, c_near, c_turn, c_far, c_both = held[:12]
    spectrum, row_fwd, row_inv, col_main, col_small = held[12:]
    state, total, z, y_hi, y_lo, w_main, w_rest, w_same, u_main, u_rest, u_same, t_main, t_rest, t_same = refs[19:33]
    left_main, left_small, right_main, right_small, scale = refs[33:38]
    w, u, t = (w_main, w_rest, w_same), (u_main, u_rest, u_same), (t_main, t_rest, t_same)
    rows, cols = state.shape
    col_windows = col_main.shape[1]
    half = row_fwd.shape[1]
    quarter = half // 2
    band_width = half - HALF
    tile_rows, tile_cols = rows // TILE, cols // TILE
    block_rows, block_cols = s_near.shape[-2:]
    near_count = s_near.shape[0]
    here_x, here_y, here_c = place[0], place[1], place[2]
    square = jnp.zeros((8, LANES), jnp.float32)
    for load in loads[:4]:
        load.wait()
    for pos in range(2 * near_count):
        s_row = (here_x ^ hx_bits[0][pos]) * block_rows
        s_row = pl.multiple_of(s_row, block_rows)
        for far, ref in enumerate((s_near, s_far) if pos < near_count else (s_turn, s_both)):
            for k in range(ref.shape[1]):
                s_col = ((here_y ^ k) * 2 + (here_c ^ far)) * block_cols
                s_col = pl.multiple_of(s_col, block_cols)
                value = ref[pos % near_count, k]
                state[pl.ds(s_row, block_rows), pl.ds(s_col, block_cols)] = value
                total[pl.ds(s_row, block_rows), pl.ds(s_col, block_cols)] = value
                square = square + jnp.sum((value * value).reshape(block_rows // 8, 8, block_cols), 0)
    for load in loads[4:8]:
        load.wait()
    share = TILE // block_rows
    for pos in range(2 * near_count):
        index = here_x ^ hx_bits[1][pos]
        a = index // share
        sub = pl.multiple_of((index % share) * block_rows, block_rows)
        for far, ref in enumerate((r_near, r_far) if pos < near_count else (r_turn, r_both)):
            side = here_c ^ far
            for k in range(ref.shape[1]):
                lane = side * (cols // 2) + k * LANES
                b = lane // TILE
                at = pl.multiple_of(lane % TILE, LANES)
                cells = ref[pos % near_count, k] * (LEFT_SCALE * mask[a, b].astype(jnp.float32))
                high, rest, same = split_small(cells)
                left_main[a, b, pl.ds(sub, block_rows), pl.ds(at, LANES)] = high
                left_small[a, b, pl.ds(sub, block_rows), pl.ds(at, LANES)] = same
                left_small[a, b, pl.ds(sub, block_rows), pl.ds(pl.multiple_of(at + TILE, LANES), LANES)] = rest
    for load in loads[8:12]:
        load.wait()
    for k in range(2 * c_near.shape[0]):
        for far, ref in enumerate((c_near, c_far) if k < c_near.shape[0] else (c_turn, c_both)):
            lane = ((here_y ^ k) * 2 + (here_c ^ far)) * block_cols
            b = lane // TILE
            at = pl.multiple_of(lane % TILE, block_cols)
            for a in range(tile_rows):
                high, rest, same = split_small(ref[k % c_near.shape[0], pl.ds(a * TILE, TILE), :] * RIGHT_SCALE)
                right_main[a, b, :, pl.ds(at, block_cols)] = high
                right_small[a, b, pl.ds(0, TILE), pl.ds(at, block_cols)] = same
                right_small[a, b, pl.ds(TILE, TILE), pl.ds(at, block_cols)] = rest

    for edge in (0, rows + band_width):
        z[pl.ds(edge, band_width), :] = jnp.zeros((band_width, z.shape[1]), jnp.float32)

    def triple(hi_ref, lo_ref, row_at, col_at, axis):
        high = hi_ref[row_at, col_at]
        return jnp.concatenate([high, lo_ref[row_at, col_at], high], axis)

    def put(refs, at, value):
        for ref, part in zip(refs, split_small(value)):
            ref[at] = part

    def scaled_by(sum_square):
        return VECTOR_SCALE * lax.rsqrt(jnp.maximum(jnp.full((8, LANES), sum_square), 1e-30))

    def times(cells, factor):
        return (cells.reshape(-1, 8, LANES) * factor).reshape(cells.shape)

    def columns(b):
        at = slice(None), pl.ds(b * HALF, TILE)
        rest_same = jnp.concatenate([w_rest[at], w_same[at]], 1)
        z[pl.ds(band_width, rows), pl.ds(b * TILE, TILE)] = dot32(w_main[at], col_main[0, b]) + dot32(
            rest_same, col_small[0, b]
        )

    def spectral(a, b, part):
        cb = pl.ds(b * TILE, TILE)
        upper = z[pl.ds(a * TILE, half), cb]
        lower = z[pl.ds(a * TILE + half, half), cb]
        high, low = split(upper - lower if part else upper + lower)
        wave = dot32(row_fwd[part], jnp.concatenate([high, low, high], 0))
        for i in (0, 1):
            for j in (0, 1):
                ri, rj = slice(i * quarter, (i + 1) * quarter), slice((1 - i) * quarter, (2 - i) * quarter)
                ci, cj = slice(j * HALF, (j + 1) * HALF), slice((1 - j) * HALF, (2 - j) * HALF)
                y = (
                    spectrum[part, 0, ri, ci] * wave[ri, ci]
                    + spectrum[part, 1, ri, ci] * wave[rj, ci]
                    + spectrum[part, 2, ri, ci] * wave[ri, cj]
                    + spectrum[part, 3, ri, ci] * wave[rj, cj]
                )
                to = pl.ds((2 * a + part) * half + i * quarter, quarter), pl.ds(b * TILE + j * HALF, HALF)
                y_hi[to], y_lo[to] = split(y)

    def back_rows(a, b):
        cb = pl.ds(b * TILE, TILE)
        sums, diffs = (
            dot32(row_inv[part], triple(y_hi, y_lo, pl.ds((2 * a + part) * half, half), cb, 0)) for part in (0, 1)
        )
        upper = sums[band_width:] + diffs[band_width:]
        lower = sums[: half - band_width] - diffs[: half - band_width]
        put(u, (pl.ds(a * TILE, HALF), cb), upper)
        put(u, (pl.ds(a * TILE + HALF, HALF), cb), lower)

    def tile_left(a, b):
        at = pl.ds(a * TILE, TILE), pl.ds(b * TILE, TILE)
        rest_same = jnp.concatenate([w_rest[at], w_same[at]], 0)
        put(t, at, dot32(left_main[a, b], w_main[at]) + dot32(left_small[a, b], rest_same))

    def update(a, keep, take, factor):
        ra = pl.ds(a * TILE, TILE)
        square = jnp.zeros((8, LANES), jnp.float32)
        before = None
        for b in range(col_windows + 1):
            done = before
            if b < col_windows:
                at = ra, pl.ds(b * TILE, TILE)
                lhs, lhs_small, rhs, rhs_small = [u_main[at]], [u_rest[at], u_same[at]], [col_main[1, b]], [col_small[1, b]]
                if b % 2 == 0:
                    at = ra, pl.ds(b // 2 * TILE, TILE)
                    lhs, lhs_small = lhs + [t_main[at]], lhs_small + [t_rest[at], t_same[at]]
                    rhs, rhs_small = rhs + [right_main[a, b // 2]], rhs_small + [right_small[a, b // 2]]
                cells = dot32(jnp.concatenate(lhs, 1), jnp.concatenate(rhs, 0)) + dot32(
                    jnp.concatenate(lhs_small, 1), jnp.concatenate(rhs_small, 0)
                )
                done = cells[:, :HALF] if before is None else before + cells[:, :HALF]
                before = cells[:, HALF:]
            cj = pl.ds(b * HALF, HALF)
            residual = keep * state[ra, cj] - times(done, take)
            state[ra, cj] = residual
            total[ra, cj] = total[ra, cj] + relax_step * residual
            put(w, (ra, cj), times(residual, factor))
            square = square + jnp.sum((residual * residual).reshape(TILE // 8, 8, LANES), 0)
        return square

    def step(k, carry):
        sums, last = carry
        keep = jnp.where(k == 0, 0.0, 1.0 - relax_step)
        take = jnp.where(k == 0, 1.0, relax_step) / (BACK_SCALE * scale[...])
        factor = scaled_by(last)
        tiles = [(a, b) for a in range(tile_rows) for b in range(tile_cols)]
        for b in range(col_windows):
            columns(b)
            if tiles:
                tile_left(*tiles.pop(0))
        for b in range(col_windows):
            for a in range(tile_rows):
                spectral(a, b, 0)
                spectral(a, b, 1)
                if tiles:
                    tile_left(*tiles.pop(0))
                if b:
                    back_rows(a, b - 1)
        for at in tiles:
            tile_left(*at)
        for a in range(tile_rows):
            back_rows(a, col_windows - 1)
        square = jnp.zeros((8, LANES), jnp.float32)
        for a in range(tile_rows):
            square = square + update(a, keep, take, factor)
        scale[...] = factor
        sum_square = jnp.sum(square)
        return jnp.where(norm_lane == k, sum_square, sums), sum_square

    sum_square = jnp.sum(square)
    scale[...] = scaled_by(sum_square)
    for i in range(0, rows, TILE):
        for j in range(0, cols, LANES):
            at = pl.ds(i, TILE), pl.ds(j, LANES)
            put(w, at, times(state[at], scale[...]))
    norm_lane = lax.broadcasted_iota(jnp.int32, norms.shape, 1)
    for load in loads[12:]:
        load.wait()
    def two_steps(k, carry):
        return step(2 * k + 1, step(2 * k, carry))

    summed, _ = lax.fori_loop(0, ITERS // 2, two_steps, (jnp.zeros(norms.shape, jnp.float32), sum_square))
    norms[...] = jnp.sqrt(summed / (rows * cols) + tiny_square)
    own_row = pl.multiple_of(here_x * block_rows, block_rows)
    own_col = pl.multiple_of((here_y * 2 + here_c) * block_cols, block_cols)
    out[...] = total[pl.ds(own_row, block_rows), pl.ds(own_col, block_cols)]


def swap(value, axis, bit):
    return lax.ppermute(value, axis, [(i, i ^ bit) for i in range(lax.axis_size(axis))])


def doubled(value, axis, bits):
    for bit in bits:
        value = jnp.concatenate([value, swap(value, axis, bit)], 0)
    return value


def bit_places(bits):
    places = [0]
    for bit in bits:
        places = places + [p | bit for p in places]
    return places


def replicated(source, coeffs, row_factor, col_factor, tile_mask):
    block_rows, block_cols = source.shape
    rows, cols = col_factor.shape[0], row_factor.shape[1]
    band_width = (coeffs.shape[0] - 1) // 2
    hx_size, hy_size = lax.axis_size("hx"), lax.axis_size("hy")
    index_x, index_y = lax.axis_index("hx"), lax.axis_index("hy")
    down = [1 << i for i in reversed(range(hx_size.bit_length() - 1))]
    turned = down[:-2] + down[-2:][::-1]
    y_bits = [1 << i for i in range(1, hy_size.bit_length() - 1)]
    s_part = doubled(source[None], "hy", y_bits)
    r_half = lax.dynamic_slice_in_dim(row_factor, (index_y % 2) * (cols // 2), cols // 2, 1)
    r_near = doubled(r_half.reshape(block_rows, -1, LANES).swapaxes(0, 1)[None], "hx", turned[:-1])
    s_near = doubled(s_part[None], "hx", down[:-2])
    s_near = doubled(s_near, "hx", down[-2:-1])
    s_near, coeffs = lax.optimization_barrier((s_near, coeffs))
    ready = setup(coeffs, cols)
    c_near = doubled(col_factor[None], "hy", y_bits[:-1])
    turns = [swap(s_near, "hx", down[-1]), swap(r_near, "hx", turned[-1]), swap(c_near, "hy", y_bits[-1])]
    s_held, *ready = lax.optimization_barrier((s_near, *ready))
    pieces = []
    for near, held, turn in zip((s_near, r_near, c_near), (s_held, r_near, c_near), turns):
        pieces += [near, turn, swap(held, "hy", 1), swap(turn, "hy", 1)]
    spectrum, col_main, col_small = ready
    row_fwd, row_inv = (jnp.asarray(m) for m in row_mats(band_width))
    place = jnp.stack([index_x, index_y // 2, index_y % 2])
    half, col_windows = HALF + band_width, cols // HALF - 1
    vmem = pl.BlockSpec(memory_space=pltpu.VMEM)
    smem = pl.BlockSpec(memory_space=pltpu.SMEM)
    f32, bf16 = jnp.float32, jnp.bfloat16
    tiles = (rows // TILE, cols // TILE)
    wide = col_windows * TILE
    shapes = [((rows, cols), f32)] * 2 + [((rows + 2 * band_width, wide), f32)]
    shapes += [((2 * half * tiles[0], wide), bf16)] * 2
    for shape in ((rows, cols), (rows, wide), (rows, cols)):
        shapes += [(shape, bf16), (shape, small), (shape, small)]
    shapes += [(tiles + (TILE, TILE), bf16), (tiles + (TILE, 2 * TILE), small)]
    shapes += [(tiles + (TILE, TILE), bf16), (tiles + (2 * TILE, TILE), small), ((8, LANES), f32)]
    operands = (*pieces, spectrum, row_fwd, row_inv, col_main, col_small)
    shapes += [(v.shape, v.dtype) for v in operands]
    result, norms = pl.pallas_call(
        functools.partial(replicated_kernel, (bit_places(down), bit_places(turned))),
        out_shape=(
            jax.ShapeDtypeStruct((block_rows, block_cols), f32),
            jax.ShapeDtypeStruct((1, ITERS), f32),
        ),
        in_specs=[smem, smem] + [pl.BlockSpec(memory_space=pl.ANY)] * 17,
        out_specs=(vmem, vmem),
        scratch_shapes=[pltpu.VMEM(*s) for s in shapes] + [pltpu.SemaphoreType.DMA((len(operands),))],
        compiler_params=pltpu.CompilerParams(vmem_limit_bytes=50432 * 1024),
        name="replicated_steps",
    )(place, tile_mask, *operands)
    return result, norms[0]


def fits(rows, cols, block_rows, block_cols, band_width, hx_size, hy_size):
    powers = all(n & (n - 1) == 0 for n in (hx_size, hy_size))
    whole = rows % TILE == 0 and cols % TILE == 0 and rows > TILE and cols > TILE
    aligned = TILE % block_rows == 0 and block_rows % 16 == 0 and block_cols == LANES and cols % (2 * LANES) == 0
    small = rows * cols * 4 <= GRID_BYTES and 4 * band_width <= TILE and band_width % 32 == 0
    return powers and whole and aligned and small and hx_size >= 4 and hy_size >= 4


def local(source, coeffs, row_factor, col_factor, tile_mask):
    rows, cols = col_factor.shape[0], row_factor.shape[1]
    band_width = (coeffs.shape[0] - 1) // 2
    sizes = lax.axis_size("hx"), lax.axis_size("hy")
    if fits(rows, cols, *source.shape, band_width, *sizes):
        return replicated(source, coeffs, row_factor, col_factor, tile_mask)
    return distributed(source, coeffs, row_factor, col_factor, tile_mask)


def solution(mesh):
    in_specs = (P("hx", "hy"), P(), P("hx", None), P(None, "hy"), P())
    out_specs = (P("hx", "hy"), P())
    return jax.shard_map(local, mesh=mesh, in_specs=in_specs, out_specs=out_specs, check_vma=False)
```
